256 devices in a mesh: row: 64 (over x, z, core), col: 4 (over y).
Axes of the slice: x: 4, y: 4, z: 8, core: 2. Of those that a mesh axis runs over, the one named last changes fastest.
Arguments:
- eigvecs: float32 [16384, 512], P('row', 'col'), may hold values from -6 to 6
- reflectors: float32 [8, 256, 128, 64], P(None, ('row', 'col')), may hold values from -2 to 2, as said below
- factors: float32 [8, 256, 64, 64], P(None, ('row', 'col')), may hold values from -3 to 3, as said below
- order: int32 [8], replicated, may hold values from 0 to 7, each once
- offsets: int32 [8], replicated, may hold values from 0 to 63
Outputs:
- rotated: float32 [16384, 512], P('row', 'col')
The draws below stay inside these ranges and needn't reach their ends.
Inputs may be any that keep to these rules, and one draw needn't show every extreme that they name: `order`: a permutation of 0 .. 7. Every block map is orthogonal: with V the block of reflectors and T the block of factors, T is upper triangular and T^-1 + T^-T = V^T V. `factors`: upper triangular, paired with reflectors as promised there.
All inputs are finite; a program needn't handle non-finite values.
Results may differ from the reference program's by a relative error of at most 0.0003.
Values sent between devices are 32-bit elements; how exact they have to be, the bound alone decides.
A program may use at most 64 MiB of HBM per device.

```python
import jax
import jax.numpy as jnp
from jax import lax

NB = 64
SWEEPS = 8
NBLK = 256
ORDER = 16384
VECS = 512


def build_pair(key):
    inner_key = jax.random.fold_in(key, 11)
    spread = 0.03
    identity = jnp.eye(NB, dtype=jnp.float32)
    base = jnp.concatenate([identity, -identity], 0)
    noise = jax.random.normal(inner_key, (SWEEPS, NBLK, 2 * NB, NB), jnp.float32) * spread
    householder = base + noise
    gram = jnp.einsum('abik,abil->abkl', householder, householder, precision=lax.Precision.HIGHEST)
    inverse_factor = jnp.triu(gram, 1) + gram * identity * 0.5
    triangle = lax.linalg.triangular_solve(inverse_factor, jnp.broadcast_to(identity, inverse_factor.shape), left_side=True, lower=False)
    return (householder, triangle)


def draw_reflectors(key, part):
    return build_pair(key)[0]


def draw_factors(key, part):
    return build_pair(key)[1]


def with_ends(drawn, own_key, smallest, top_value):
    longest = drawn.shape.index(max(drawn.shape))
    spots = []
    for shift in (0, 1):
        where = [jax.random.randint(jax.random.fold_in(own_key, axis), (), 0, length) for axis, length in enumerate(drawn.shape)]
        where[longest] = (where[longest] + shift) % drawn.shape[longest]
        spots.append(tuple(where))
    return drawn.at[spots[0]].set(smallest).at[spots[1]].set(top_value)


def block_scale(stream_key, extent, cuts, least, largest):
    def one(dim, shards_of):
        heights = jax.random.uniform(jax.random.fold_in(jax.random.fold_in(stream_key, 6), dim), (shards_of,), jnp.float32, least / len(cuts), largest / len(cuts))
        return jnp.repeat(jnp.exp(heights), extent[dim] // shards_of).reshape((-1,) + (1,) * (len(extent) - dim - 1))

    loudness = one(*cuts[0])
    for cut in cuts[1:]:
        loudness = loudness * one(*cut)
    return loudness


def centred(stream_key, extent, scale, limit, split=(), kind=jnp.bfloat16):
    factor_of = block_scale(stream_key, extent, split, -0.22, 0.18) if split else 1.0
    entries = jax.random.normal(stream_key, extent, jnp.float32) * scale * factor_of
    return jnp.minimum(jnp.maximum(entries, -limit), limit).astype(kind)


def setup_inputs(seed: int = 0) -> dict:
    key_list = jax.random.split(jax.random.key(seed), 6)
    return {
        "eigvecs": centred(key_list[0], (ORDER, VECS), 1.0, 6.0, ((0, 64), (1, 4)), jnp.float32),
        "reflectors": draw_reflectors(jax.random.fold_in(key_list[5], 71), 0),
        "factors": draw_factors(jax.random.fold_in(key_list[5], 71), 0),
        "order": jax.random.permutation(key_list[3], SWEEPS).astype(jnp.int32),
        "offsets": with_ends(jax.random.randint(key_list[4], (SWEEPS,), 0, NB), jax.random.fold_in(key_list[4], 1), 0, NB - 1).astype(jnp.int32),
    }


highest = lax.Precision.HIGHEST

def reflect(segment, householder, triangle):
    inner = jnp.dot(householder.T.astype(jnp.float32), segment.astype(jnp.float32), precision=highest, preferred_element_type=jnp.float32)
    inner = jnp.dot(triangle.astype(jnp.float32), inner.astype(jnp.float32), precision=highest, preferred_element_type=jnp.float32)
    return segment - jnp.dot(householder.astype(jnp.float32), inner.astype(jnp.float32), precision=highest, preferred_element_type=jnp.float32)

def reference(eigvecs, reflectors, factors, order, offsets):
    height = eigvecs.shape[0]
    columns = eigvecs.shape[1]
    number_blocks = reflectors.shape[1]
    vectors = eigvecs
    for position in range(SWEEPS):
        stored = order[position].astype(jnp.int32)
        offset = offsets[stored].astype(jnp.int32)
        house_set = lax.dynamic_index_in_dim(reflectors, stored, 0, keepdims=False)
        tri_set = lax.dynamic_index_in_dim(factors, stored, 0, keepdims=False)
        padded = jnp.concatenate([vectors, jnp.zeros((2 * NB, columns), jnp.float32)], 0)

        def advance(number, current):
            start = (offset + number * NB).astype(jnp.int32)
            segment = lax.dynamic_slice_in_dim(current, start, 2 * NB, 0)
            householder = lax.dynamic_index_in_dim(house_set, number, 0, keepdims=False)
            triangle = lax.dynamic_index_in_dim(tri_set, number, 0, keepdims=False)
            return lax.dynamic_update_slice_in_dim(current, reflect(segment, householder, triangle), start, 0)
        padded = lax.fori_loop(0, number_blocks, advance, padded)
        vectors = padded[:height]
    return vectors
```

```python
import functools

import jax
import jax.numpy as jnp
from jax import lax
from jax.experimental import pallas as pl
from jax.experimental.pallas import tpu as pltpu
from jax.sharding import Mesh
from jax.sharding import PartitionSpec as P

ROW = ("x", "z", "core")
ROW_COL = ("x", "z", "core", "y")
MESH = pl.DeviceIdType.MESH
F32 = jnp.float32
BF16 = jnp.bfloat16
NB = 64
HI = lax.Precision.HIGHEST
VM = pltpu.VMEM


def dot_f32(a, b):
    return jnp.dot(a, b, precision=HI, preferred_element_type=F32)


def halves(a):
    high = a.astype(BF16)
    return high, (a - high.astype(F32)).astype(BF16)


def dot3(a_high, a_low, b_high, b_low):
    product = functools.partial(jnp.dot, preferred_element_type=F32)
    return product(a_high, b_high) + (product(a_high, b_low) + product(a_low, b_high))


def packed(a):
    n = a.shape[0] // 2
    return jnp.concatenate([a[:n], a[n:]], axis=1)


def unpacked(a):
    return jnp.concatenate([a[:, :NB], a[:, NB:]], axis=0)


def beside(a, b):
    return jnp.concatenate([a, b], axis=1)


def barrier(devices):
    semaphore = pltpu.get_barrier_semaphore()
    for device in devices:
        pl.semaphore_signal(semaphore, inc=1, device_id=device, device_id_type=MESH)
    pl.semaphore_wait(semaphore, len(devices))


def remote(source, target, sent, received, device):
    return pltpu.make_async_remote_copy(
        src_ref=source, dst_ref=target, send_sem=sent, recv_sem=received, device_id=device, device_id_type=MESH
    )


def gather_kernel(vt_ref, t_ref, gv_ref, gt_ref, tp_ref, sent, received):
    y = lax.axis_index("y")
    right, left, across = lax.rem(y + 1, 4), lax.rem(y + 3, 4), lax.rem(y + 2, 4)
    barrier([{"y": right}, {"y": left}])
    sends = []

    def start(source, target, k, side):
        copy = remote(source, target, sent.at[k], received.at[k], {"y": side})
        copy.start()
        sends.append(copy)

    start(vt_ref, gv_ref.at[y], 0, right)
    start(vt_ref, gv_ref.at[y], 1, left)
    half = t_ref.shape[0] // 2
    for k in range(half):
        tp_ref[k] = beside(t_ref[2 * k], t_ref[2 * k + 1])
    start(tp_ref, gt_ref.at[y], 2, right)
    start(tp_ref, gt_ref.at[y], 3, left)
    gv_ref[y] = vt_ref[...]
    gt_ref[y] = tp_ref[...]

    def arrived(target, k):
        remote(target, target, sent.at[k], received.at[k], {"y": right}).wait_recv()

    lower, upper = pl.ds(0, half), pl.ds(half, half)
    arrived(gv_ref.at[left], 0)
    start(gv_ref.at[left, lower], gv_ref.at[left, lower], 4, right)
    arrived(gv_ref.at[right], 1)
    start(gv_ref.at[right, upper], gv_ref.at[right, upper], 5, left)
    lower_t, upper_t = pl.ds(0, half // 2), pl.ds(half // 2, half // 2)
    arrived(gt_ref.at[left], 2)
    start(gt_ref.at[left, lower_t], gt_ref.at[left, lower_t], 6, right)
    arrived(gt_ref.at[right], 3)
    start(gt_ref.at[right, upper_t], gt_ref.at[right, upper_t], 7, left)
    arrived(gv_ref.at[across, lower], 4)
    arrived(gv_ref.at[across, upper], 5)
    arrived(gt_ref.at[across, lower_t], 6)
    arrived(gt_ref.at[across, upper_t], 7)
    for copy in sends:
        copy.wait_send()


def gather_blocks(vt, t):
    sweeps = vt.shape[0]
    return pl.pallas_call(
        gather_kernel,
        out_shape=[
            jax.ShapeDtypeStruct((4, sweeps, NB, 2 * NB), F32),
            jax.ShapeDtypeStruct((4, sweeps // 2, NB, 2 * NB), F32),
        ],
        in_specs=[pl.BlockSpec(memory_space=VM)] * 2,
        out_specs=[pl.BlockSpec(memory_space=VM)] * 2,
        scratch_shapes=[
            VM((sweeps // 2, NB, 2 * NB), F32),
            pltpu.SemaphoreType.DMA((8,)),
            pltpu.SemaphoreType.DMA((8,)),
        ],
        compiler_params=pltpu.CompilerParams(collective_id=0, has_side_effects=True),
        name="gather_blocks",
    )(vt, t)


def build_kernel(order_ref, gv_ref, gt_ref, out_ref):
    stored = order_ref[pl.program_id(0)]
    odd = lax.rem(stored, 2) == 1
    eye = (
        lax.broadcasted_iota(jnp.int32, (2 * NB, 2 * NB), 0) == lax.broadcasted_iota(jnp.int32, (2 * NB, 2 * NB), 1)
    ).astype(F32)
    carry = None
    for j in range(4):
        vt = gv_ref[j, 0]
        pair = gt_ref[j, 0]
        t = jnp.where(odd, pair[:, NB:], pair[:, :NB])
        w = dot_f32(t, vt)
        block = eye - lax.dot_general(vt, w, (((0,), (0,)), ((), ())), precision=HI, preferred_element_type=F32)
        if j == 0:
            rows = block
        else:
            rows = beside(dot_f32(block[:, :NB], carry), block[:, NB:])
        wide = rows.shape[1]
        out_ref[0, NB * j : NB * (j + 1), :] = jnp.concatenate(
            [rows[:NB], jnp.zeros((NB, 6 * NB - wide), F32)], axis=1
        )
        carry = rows[NB:]
    out_ref[0, 4 * NB :, :] = beside(carry, jnp.zeros((NB, NB), F32))


def build_maps(order, gv, gt):
    sweeps = gv.shape[1]
    return pl.pallas_call(
        build_kernel,
        out_shape=jax.ShapeDtypeStruct((sweeps, 5 * NB, 6 * NB), F32),
        grid_spec=pltpu.PrefetchScalarGridSpec(
            num_scalar_prefetch=1,
            grid=(sweeps,),
            in_specs=[
                pl.BlockSpec((4, 1, NB, 2 * NB), lambda p, order: (0, order[p], 0, 0)),
                pl.BlockSpec((4, 1, NB, 2 * NB), lambda p, order: (0, order[p] // 2, 0, 0)),
            ],
            out_specs=pl.BlockSpec((1, 5 * NB, 6 * NB), lambda p, order: (p, 0, 0)),
        ),
        name="build_maps",
    )(order, gv, gt)


class Place:
    def __init__(self):
        self.nx, self.nz = lax.axis_size("x"), lax.axis_size("z")
        self.x, self.z, self.core = lax.axis_index("x"), lax.axis_index("z"), lax.axis_index("core")
        chips = self.nx * self.nz
        self.chip = self.x * self.nz + self.z
        following, before = lax.rem(self.chip + 1, chips), lax.rem(self.chip + chips - 1, chips)
        self.following = {"x": following // self.nz, "z": lax.rem(following, self.nz)}
        self.before = {"x": before // self.nz, "z": lax.rem(before, self.nz)}
        self.partner = {"core": 1 - self.core}
        self.first = self.chip == 0
        self.last = self.chip == chips - 1

    def z_peers(self):
        return [{"z": lax.rem(self.z + d, self.nz)} for d in range(1, self.nz)]

    def x_peers(self):
        return [{"x": lax.rem(self.x + d, self.nx)} for d in range(1, self.nx)]

    def greet(self):
        barrier([self.partner, self.following, self.before] + self.z_peers() + self.x_peers())


def prepare_kernel(
    own_ref, mh_ref, ml_ref, reh_ref, rel_ref, rhh_ref, rhl_ref, pzh_ref, pzl_ref, pxh_ref, pxl_ref,
    other_ref, resp_ref, head_ref, next_ref, tz_ref, tx_ref, pz_ref, px_ref, sent, received, sent_z, received_z, sent_x, received_x,
):
    here = Place()
    nx, nz, core = here.nx, here.nz, here.core
    sweeps = own_ref.shape[0]
    mine = sweeps // 2
    here.greet()
    sends = []

    def start(source, target, send_sem, recv_sem, device):
        copy = remote(source, target, send_sem, recv_sem, device)
        copy.start()
        sends.append(copy)

    def arrived(target, send_sem, recv_sem):
        remote(target, target, send_sem, recv_sem, here.partner).wait_recv()

    start(own_ref, other_ref, sent.at[0], received.at[0], here.partner)

    def split_own(p, _):
        high, low = halves(own_ref[p])
        mh_ref[core, p] = high
        ml_ref[core, p] = low
        return 0

    lax.fori_loop(0, sweeps, split_own, 0)
    arrived(other_ref, sent.at[0], received.at[0])

    def respond(p, _):
        high, low = halves(other_ref[p])
        mh_ref[1 - core, p] = high
        ml_ref[1 - core, p] = low
        mine_first, other_first = own_ref[p, :, : 2 * NB], other_ref[p, :, : 2 * NB]
        first = jnp.where(core == 0, mine_first, other_first)[:, :NB]
        second = jnp.where(core == 0, other_first, mine_first)[:, :NB]
        resp_ref[p, : 4 * NB] = first[: 4 * NB]
        resp_ref[p, 4 * NB :] = dot_f32(second, first[4 * NB :])
        head_ref[p] = packed(first[: 2 * NB])
        return 0

    lax.fori_loop(0, sweeps, respond, 0)
    for k in range(mine // 2):
        p = mine * core + 2 * k
        tz_ref[here.z, k] = beside(resp_ref[p, 8 * NB :], resp_ref[p + 1, 8 * NB :])
    for d in range(1, nz):
        start(tz_ref.at[here.z], tz_ref.at[here.z], sent_z.at[d], received_z.at[here.z], {"z": lax.rem(here.z + d, nz)})
    start(head_ref, next_ref, sent.at[1], received.at[1], here.before)
    for d in range(1, nz):
        slot = lax.rem(here.z + d, nz)
        arrived(tz_ref.at[slot], sent_z.at[d], received_z.at[slot])

    eye = (lax.broadcasted_iota(jnp.int32, (NB, NB), 0) == lax.broadcasted_iota(jnp.int32, (NB, NB), 1)).astype(F32)

    def piece(ref, slot, k):
        pair = ref[slot, k // 2]
        return pair[:, NB:] if k % 2 else pair[:, :NB]

    whole, reach = [], []
    for k in range(mine):
        p = mine * core + k
        upto = jnp.zeros((NB, NB), F32)
        full = eye
        for slot in reversed(range(nz)):
            if slot < nz - 1:
                both = dot_f32(jnp.concatenate([upto, full], axis=0), piece(tz_ref, slot + 1, k))
                upto, full = both[:NB], both[NB:]
            upto = jnp.where(slot == here.z - 1, eye, upto)
            both = jnp.concatenate([upto, full], axis=0)
            at = slice(NB // 2 * slot, NB // 2 * (slot + 1))
            pz_ref[p, : 2 * NB, at] = both[:, : NB // 2]
            pz_ref[p, 2 * NB :, at] = both[:, NB // 2 :]
        both = dot_f32(jnp.concatenate([upto, full], axis=0), piece(tz_ref, 0, k))
        reach.append(jnp.where(here.z == 0, eye, both[:NB]))
        whole.append(both[NB:])
    for k in range(mine // 2):
        tx_ref[here.x, k] = beside(whole[2 * k], whole[2 * k + 1])
    for d in range(1, nx):
        start(tx_ref.at[here.x], tx_ref.at[here.x], sent_x.at[d], received_x.at[here.x], {"x": lax.rem(here.x + d, nx)})
    positions = pl.ds(mine * core, mine)
    start(pz_ref.at[positions], pz_ref.at[positions], sent.at[2], received.at[2], here.partner)

    arrived(next_ref, sent.at[1], received.at[1])

    def extend(p, _):
        ahead = unpacked(next_ref[p])
        rhh_ref[p], rhl_ref[p] = halves(ahead)
        resp = resp_ref[p]
        reh_ref[p, : 8 * NB], rel_ref[p, : 8 * NB] = halves(resp[: 8 * NB])
        reh_ref[p, 8 * NB :], rel_ref[p, 8 * NB :] = halves(dot_f32(ahead, resp[8 * NB :]))
        return 0

    lax.fori_loop(0, sweeps, extend, 0)

    for d in range(1, nx):
        slot = lax.rem(here.x + d, nx)
        arrived(tx_ref.at[slot], sent_x.at[d], received_x.at[slot])
    for k in range(mine):
        p = mine * core + k
        upto = jnp.zeros((NB, NB), F32)
        for slot in reversed(range(nx)):
            if slot < nx - 1:
                upto = dot_f32(upto, piece(tx_ref, slot + 1, k))
            upto = jnp.where(slot == here.x - 1, reach[k], upto)
            at = slice(NB // 2 * slot, NB // 2 * (slot + 1))
            px_ref[p, :NB, at] = upto[:, : NB // 2]
            px_ref[p, NB:, at] = upto[:, NB // 2 :]
    start(px_ref.at[positions], px_ref.at[positions], sent.at[3], received.at[3], here.partner)
    others = pl.ds(mine * (1 - core), mine)
    arrived(pz_ref.at[others], sent.at[2], received.at[2])
    arrived(px_ref.at[others], sent.at[3], received.at[3])

    def split_carry(p, _):
        pzh_ref[p], pzl_ref[p] = halves(pz_ref[p])
        pxh_ref[p], pxl_ref[p] = halves(px_ref[p])
        return 0

    lax.fori_loop(0, sweeps, split_carry, 0)
    for copy in sends:
        copy.wait_send()


def prepare(maps, nx, nz):
    sweeps = maps.shape[0]
    half = NB // 2

    def pair(*shape):
        return [jax.ShapeDtypeStruct(shape, BF16)] * 2

    outs = (
        pair(2, sweeps, 5 * NB, 6 * NB)
        + pair(sweeps, 10 * NB, NB)
        + pair(sweeps, 2 * NB, NB)
        + pair(sweeps, 4 * NB, half * nz)
        + pair(sweeps, 2 * NB, half * nx)
    )
    return pl.pallas_call(
        prepare_kernel,
        out_shape=outs,
        in_specs=[pl.BlockSpec(memory_space=VM)],
        out_specs=[pl.BlockSpec(memory_space=VM)] * len(outs),
        scratch_shapes=[
            VM(maps.shape, F32),
            VM((sweeps, 9 * NB, NB), F32),
            VM((sweeps, NB, 2 * NB), F32),
            VM((sweeps, NB, 2 * NB), F32),
            VM((nz, sweeps // 4, NB, 2 * NB), F32),
            VM((nx, sweeps // 4, NB, 2 * NB), F32),
            VM((sweeps, 4 * NB, half * nz), F32),
            VM((sweeps, 2 * NB, half * nx), F32),
            pltpu.SemaphoreType.DMA((4,)),
            pltpu.SemaphoreType.DMA((4,)),
            pltpu.SemaphoreType.DMA((nz,)),
            pltpu.SemaphoreType.DMA((nz,)),
            pltpu.SemaphoreType.DMA((nx,)),
            pltpu.SemaphoreType.DMA((nx,)),
        ],
        compiler_params=pltpu.CompilerParams(
            collective_id=1, has_side_effects=True, vmem_limit_bytes=60 * 1024 * 1024
        ),
        name="prepare",
    )(maps)


ABOVE = 2 * NB
OWN = 8 * NB


def sweep_kernel(
    shifts_ref, eig_ref, mh_ref, ml_ref, reh_ref, rel_ref, rhh_ref, rhl_ref, pzh_ref, pzl_ref, pxh_ref, pxl_ref, out_ref,
    rows_ref, turn_ref, turned_ref, edge_ref, edges_ref, sums_ref, totals_ref, ends_ref, heads_ref, y_ref,
    sent, received, sent_z, received_z, sent_x, received_x, sent_h, received_h,
):
    here = Place()
    nx, nz, core = here.nx, here.nz, here.core
    sweeps = mh_ref.shape[1]
    here.greet()

    def arrived(target, send_sem, recv_sem):
        remote(target, target, send_sem, recv_sem, here.partner).wait_recv()

    mine = eig_ref[...]
    turned = jnp.where(core == 0, mine, pltpu.roll(mine, NB, 1))
    turn_ref[...] = packed(turned[:, NB:])
    to_partner = remote(turn_ref, turned_ref.at[0], sent.at[0], received.at[0], here.partner)
    to_partner.start()
    rows_ref[...] = jnp.zeros_like(rows_ref)
    kept = turned[:, :NB]
    arrived(turned_ref.at[0], sent.at[0], received.at[0])
    got = unpacked(turned_ref[0])
    rows_ref[ABOVE : ABOVE + OWN] = jnp.concatenate(
        [jnp.where(core == 0, kept, got), jnp.where(core == 0, got, kept)], axis=0
    )
    edge_ref[sweeps] = packed(rows_ref[ABOVE : ABOVE + 2 * NB])
    to_before = remote(edge_ref.at[sweeps], edges_ref.at[sweeps], sent_h.at[sweeps], received_h.at[sweeps], here.before)
    to_before.start()
    arrived(edges_ref.at[sweeps], sent_h.at[sweeps], received_h.at[sweeps])
    rows_ref[ABOVE + OWN : ABOVE + OWN + 2 * NB] = unpacked(edges_ref[sweeps])
    to_partner.wait_send()
    to_before.wait_send()

    index = lax.broadcasted_iota(jnp.int32, (10 * NB, NB), 0)

    def sweep(p, _):
        shift = shifts_ref[p, 0]
        offset = shifts_ref[p, 1]
        window = rows_ref[pl.ds(NB + shift, 10 * NB), :]
        beyond = jnp.logical_and(here.last, index >= 9 * NB - offset)
        carried = jnp.logical_and(jnp.logical_not(here.first), jnp.logical_and(index >= NB, index < 2 * NB))
        inputs = jnp.where(jnp.logical_or(beyond, carried), 0.0, window)
        head = window[:NB]
        high, low = halves(inputs[NB : 7 * NB])
        end_a = dot3(mh_ref[0, p, 4 * NB :], ml_ref[0, p, 4 * NB :], high, low)
        second = jnp.concatenate([end_a, inputs[6 * NB :], jnp.zeros((NB, NB), F32)], axis=0)
        high_b, low_b = halves(second)
        end_b = dot3(mh_ref[1, p, 4 * NB :], ml_ref[1, p, 4 * NB :], high_b, low_b)
        sums_ref[p, here.z] = packed(end_b)
        z_copies = []
        for d in range(1, nz):
            copy = remote(
                sums_ref.at[p, here.z], sums_ref.at[p, here.z], sent_z.at[p, d], received_z.at[p, here.z],
                {"z": lax.rem(here.z + d, nz)},
            )
            copy.start()
            z_copies.append(copy)
        body_a = dot3(mh_ref[0, p, : 4 * NB], ml_ref[0, p, : 4 * NB], high, low)
        edge_ref[p] = packed(body_a[: 2 * NB])
        h_copy = remote(edge_ref.at[p], edges_ref.at[p], sent_h.at[p], received_h.at[p], here.before)
        h_copy.start()
        y_ref[: 4 * NB] = body_a
        y_ref[4 * NB : 8 * NB] = dot3(mh_ref[1, p, : 4 * NB], ml_ref[1, p, : 4 * NB], high_b, low_b)
        end_high, end_low = halves(end_b)
        ahead = dot3(rhh_ref[p], rhl_ref[p], end_high, end_low)
        for d in range(1, nz):
            slot = lax.rem(here.z + d, nz)
            arrived(sums_ref.at[p, slot], sent_z.at[p, d], received_z.at[p, slot])
        high_z, low_z = halves(sums_ref[p].reshape(nz * NB // 2, 2 * NB))
        both = dot3(pzh_ref[p], pzl_ref[p], high_z, low_z)
        combined = both[: 2 * NB, :NB] + both[2 * NB :, NB:]
        totals_ref[p, here.x] = packed(combined[NB:])
        x_copies = []
        for d in range(1, nx):
            copy = remote(
                totals_ref.at[p, here.x], totals_ref.at[p, here.x], sent_x.at[p, d], received_x.at[p, here.x],
                {"x": lax.rem(here.x + d, nx)},
            )
            copy.start()
            x_copies.append(copy)
        arrived(edges_ref.at[p], sent_h.at[p], received_h.at[p])
        y_ref[8 * NB :] = unpacked(edges_ref[p]) + ahead
        rows_ref[NB:ABOVE] = head
        for d in range(1, nx):
            slot = lax.rem(here.x + d, nx)
            arrived(totals_ref.at[p, slot], sent_x.at[p, d], received_x.at[p, slot])
        high_x, low_x = halves(totals_ref[p].reshape(nx * NB // 2, 2 * NB))
        both = dot3(pxh_ref[p], pxl_ref[p], high_x, low_x)
        carry = combined[:NB] + both[:NB, :NB] + both[NB:, NB:]
        carry_high, carry_low = halves(carry)
        rows_ref[ABOVE : ABOVE + 10 * NB] = y_ref[...] + dot3(reh_ref[p], rel_ref[p], carry_high, carry_low)
        for copy in z_copies + x_copies + [h_copy]:
            copy.wait_send()
        return 0

    lax.fori_loop(0, sweeps, sweep, 0)

    ends_ref[...] = packed(rows_ref[ABOVE + 7 * NB : ABOVE + 8 * NB])
    to_next = remote(ends_ref, heads_ref, sent.at[1], received.at[1], here.following)
    to_next.start()
    arrived(heads_ref, sent.at[1], received.at[1])
    rows_ref[NB:ABOVE] = jnp.where(here.first, rows_ref[NB:ABOVE], unpacked(heads_ref[...]))
    final = rows_ref[pl.ds(ABOVE - shifts_ref[sweeps - 1, 1], OWN), :]
    upper, lower = final[: 4 * NB], final[4 * NB :]
    turn_ref[...] = packed(jnp.where(core == 0, lower, upper))
    back = remote(turn_ref, turned_ref.at[1], sent.at[2], received.at[2], here.partner)
    back.start()
    kept = jnp.where(core == 0, upper, lower)
    arrived(turned_ref.at[1], sent.at[2], received.at[2])
    got = unpacked(turned_ref[1])
    out_ref[...] = beside(jnp.where(core == 0, kept, got), jnp.where(core == 0, got, kept))
    to_next.wait_send()
    back.wait_send()


def apply_sweeps(shifts, eigvecs, prepared, nx, nz):
    sweeps = shifts.shape[0]
    half = NB // 2
    dma = pltpu.SemaphoreType.DMA
    return pl.pallas_call(
        sweep_kernel,
        out_shape=jax.ShapeDtypeStruct(eigvecs.shape, F32),
        in_specs=[pl.BlockSpec(memory_space=pltpu.SMEM)] + [pl.BlockSpec(memory_space=VM)] * (1 + len(prepared)),
        out_specs=pl.BlockSpec(memory_space=VM),
        scratch_shapes=[
            VM((14 * NB, NB), F32),
            VM((2 * NB, 2 * NB), F32),
            VM((2, 2 * NB, 2 * NB), F32),
            VM((sweeps + 1, NB, 2 * NB), F32),
            VM((sweeps + 1, NB, 2 * NB), F32),
            VM((sweeps, nz, half, 2 * NB), F32),
            VM((sweeps, nx, half, 2 * NB), F32),
            VM((half, 2 * NB), F32),
            VM((half, 2 * NB), F32),
            VM((10 * NB, NB), F32),
            dma((3,)),
            dma((3,)),
            dma((sweeps, nz)),
            dma((sweeps, nz)),
            dma((sweeps, nx)),
            dma((sweeps, nx)),
            dma((sweeps + 1,)),
            dma((sweeps + 1,)),
        ],
        compiler_params=pltpu.CompilerParams(
            collective_id=2, has_side_effects=True, vmem_limit_bytes=60 * 1024 * 1024
        ),
        name="apply_sweeps",
    )(shifts, eigvecs, *prepared)


def solution(mesh):
    nz, cores, ny = 8, 2, mesh.shape["col"]
    nx = mesh.shape["row"] // (nz * cores)
    torus = Mesh(mesh.devices.reshape(nx, nz, cores, ny), ROW_COL)

    def local(eigvecs, reflectors, factors, order, offsets):
        transposed = jnp.swapaxes(reflectors[:, 0], 1, 2)
        gv, gt = gather_blocks(transposed, factors[:, 0])
        maps = build_maps(order, gv, gt)
        prepared = prepare(maps, nx, nz)
        used = offsets[order]
        previous = jnp.concatenate([jnp.zeros((1,), jnp.int32), used[:-1]])
        shifts = jnp.stack([used - previous, used], axis=1)
        return apply_sweeps(shifts, eigvecs, prepared, nx, nz)

    placed = (P(ROW, "y"), P(None, ROW_COL, None, None), P(None, ROW_COL, None, None), P(), P())
    return jax.shard_map(local, mesh=torus, in_specs=placed, out_specs=P(ROW, "y"), check_vma=False)
```

```python
import functools

import jax
import jax.numpy as jnp
from jax import lax
from jax.experimental import pallas as pl
from jax.experimental.pallas import tpu as pltpu
from jax.sharding import Mesh
from jax.sharding import PartitionSpec as P

ROW = ("x", "z", "core")
ROW_COL = ("x", "z", "core", "y")
MESH = pl.DeviceIdType.MESH
F32 = jnp.float32
BF16 = jnp.bfloat16
NB = 64
VM = pltpu.VMEM


def halves(a):
    high = a.astype(BF16)
    return high, (a - high.astype(F32)).astype(BF16)


def dot3(a_high, a_low, b_high, b_low):
    product = functools.partial(jnp.dot, preferred_element_type=F32)
    return product(a_high, b_high) + (product(a_high, b_low) + product(a_low, b_high))


def dot_split(a, b):
    return dot3(*halves(a), *halves(b))


def packed(a):
    n = a.shape[0] // 2
    return jnp.concatenate([a[:n], a[n:]], axis=1)


def unpacked(a):
    return jnp.concatenate([a[:, :NB], a[:, NB:]], axis=0)


def beside(a, b):
    return jnp.concatenate([a, b], axis=1)


def barrier(devices):
    semaphore = pltpu.get_barrier_semaphore()
    for device in devices:
        pl.semaphore_signal(semaphore, inc=1, device_id=device, device_id_type=MESH)
    pl.semaphore_wait(semaphore, len(devices))


def remote(source, target, sent, received, device):
    return pltpu.make_async_remote_copy(
        src_ref=source, dst_ref=target, send_sem=sent, recv_sem=received, device_id=device, device_id_type=MESH
    )


class Place:
    def __init__(self):
        self.nx, self.nz = lax.axis_size("x"), lax.axis_size("z")
        self.x, self.z, self.core = lax.axis_index("x"), lax.axis_index("z"), lax.axis_index("core")
        chips = self.nx * self.nz
        self.chip = self.x * self.nz + self.z
        following, before = lax.rem(self.chip + 1, chips), lax.rem(self.chip + chips - 1, chips)
        self.following = {"x": following // self.nz, "z": lax.rem(following, self.nz)}
        self.before = {"x": before // self.nz, "z": lax.rem(before, self.nz)}
        self.partner = {"core": 1 - self.core}
        self.first = self.chip == 0
        self.last = self.chip == chips - 1

    def z_peers(self):
        return [{"z": lax.rem(self.z + d, self.nz)} for d in range(1, self.nz)]

    def x_peers(self):
        return [{"x": lax.rem(self.x + d, self.nx)} for d in range(1, self.nx)]

    def y_peers(self):
        return [{"y": lax.rem(lax.axis_index("y") + d, 4)} for d in range(1, 4)]

    def greet(self):
        barrier([self.partner, self.following, self.before] + self.z_peers() + self.x_peers() + self.y_peers())


ABOVE = 2 * NB
OWN = 8 * NB
HALF = NB // 2


def sweeps_kernel(
    order_ref, offsets_ref, eig_ref, vt_ref, t_ref, out_ref,
    blocks_ref, own_ref, other_ref, mh_ref, ml_ref, resp_ref, reh_ref, rel_ref, head_ref, next_ref, rhh_ref, rhl_ref,
    tz_ref, tx_ref, reach_ref, pzh_ref, pzl_ref, pxh_ref, pxl_ref,
    rows_ref, turn_ref, turned_ref, edge_ref, edges_ref, sums_ref, totals_ref, ends_ref, y_ref,
    sent_y, received_y, sent_m, received_m, sent_n, received_n, sent_tz, received_tz, sent_tx, received_tx,
    sent, received, sent_z, received_z, sent_x, received_x, sent_h, received_h,
):
    here = Place()
    nx, nz, core, y = here.nx, here.nz, here.core, lax.axis_index("y")
    sweeps = vt_ref.shape[0]
    far = sorted(range(1, nz), key=lambda d: -min(d, nz - d))
    here.greet()

    def arrived(target, send_sem, recv_sem):
        remote(target, target, send_sem, recv_sem, here.partner).wait_recv()


    def block_copy(p, d):
        at = blocks_ref.at[y, p]
        return remote(at, at, sent_y.at[p, d], received_y.at[p, y], {"y": lax.rem(y + d, 4)})

    def map_copy(p):
        return remote(own_ref.at[p], other_ref.at[p], sent_m.at[p], received_m.at[p], here.partner)

    def head_copy(p):
        return remote(head_ref.at[p], next_ref.at[p], sent_n.at[p], received_n.at[p], here.before)

    def along_z(ref, p, d, send_sems, recv_sems):
        at = ref.at[p, here.z]
        return remote(at, at, send_sems.at[p, d], recv_sems.at[p, here.z], {"z": lax.rem(here.z + d, nz)})

    def along_x(ref, p, d, send_sems, recv_sems):
        at = ref.at[p, here.x]
        return remote(at, at, send_sems.at[p, d], recv_sems.at[p, here.x], {"x": lax.rem(here.x + d, nx)})

    def edge_copy(p):
        return remote(edge_ref.at[p], edges_ref.at[p], sent_h.at[p], received_h.at[p], here.before)

    def await_z(ref, p, send_sems, recv_sems):
        for d in range(1, nz):
            slot = lax.rem(here.z + d, nz)
            arrived(ref.at[p, slot], send_sems.at[p, d], recv_sems.at[p, slot])

    def await_x(ref, p, send_sems, recv_sems):
        for d in range(1, nx):
            slot = lax.rem(here.x + d, nx)
            arrived(ref.at[p, slot], send_sems.at[p, d], recv_sems.at[p, slot])


    eye = (lax.broadcasted_iota(jnp.int32, (NB, NB), 0) == lax.broadcasted_iota(jnp.int32, (NB, NB), 1)).astype(F32)
    wide_eye = (
        lax.broadcasted_iota(jnp.int32, (2 * NB, 2 * NB), 0) == lax.broadcasted_iota(jnp.int32, (2 * NB, 2 * NB), 1)
    ).astype(F32)

    def build(p):
        for d in range(1, 4):
            slot = lax.rem(y + d, 4)
            arrived(blocks_ref.at[slot, p], sent_y.at[p, d], received_y.at[p, slot])
        maps = []
        for j in range(4):
            vt = blocks_ref[j, p, :NB]
            t = unpacked(blocks_ref[j, p, NB:])
            vh, vl = halves(vt)
            wh, wl = halves(dot3(*halves(t), vh, vl))
            product = functools.partial(
                lax.dot_general, dimension_numbers=(((0,), (0,)), ((), ())), preferred_element_type=F32
            )
            maps.append(wide_eye - (product(vh, wh) + (product(vh, wl) + product(vl, wh))))
        carry = None
        for j in range(4):
            block = maps[j]
            rows = block if j == 0 else beside(dot_split(block[:, :NB], carry), block[:, NB:])
            done = jnp.concatenate([rows[:NB], jnp.zeros((NB, 6 * NB - rows.shape[1]), F32)], axis=1)
            own_ref[p, NB * j : NB * (j + 1), :] = done
            carry = rows[NB:]
        own_ref[p, 4 * NB :, :] = beside(carry, jnp.zeros((NB, NB), F32))
        map_copy(p).start()
        mh_ref[core, p], ml_ref[core, p] = halves(own_ref[p])

    def respond(p):
        arrived(other_ref.at[p], sent_m.at[p], received_m.at[p])
        mine_first, other_first = own_ref[p, :, : 2 * NB], other_ref[p, :, : 2 * NB]
        first = jnp.where(core == 0, mine_first, other_first)[:, :NB]
        second = jnp.where(core == 0, other_first, mine_first)[:, :NB]
        later = dot_split(second, first[4 * NB :])
        tz_ref[p, here.z] = packed(later[4 * NB :])
        for d in far:
            along_z(tz_ref, p, d, sent_tz, received_tz).start()
        head_ref[p] = packed(first[: 2 * NB])
        head_copy(p).start()
        resp_ref[p] = later[4 * NB :]
        reh_ref[p, : 4 * NB], rel_ref[p, : 4 * NB] = halves(first[: 4 * NB])
        reh_ref[p, 4 * NB : 8 * NB], rel_ref[p, 4 * NB : 8 * NB] = halves(later[: 4 * NB])
        mh_ref[1 - core, p], ml_ref[1 - core, p] = halves(other_ref[p])

    def chain_z(p):
        await_z(tz_ref, p, sent_tz, received_tz)
        both = jnp.concatenate([jnp.zeros((NB, NB), F32), eye], axis=0)
        upper = lax.broadcasted_iota(jnp.int32, (2 * NB, NB), 0) < NB
        twice = jnp.concatenate([eye, eye], axis=0)
        for slot in reversed(range(nz)):
            if slot < nz - 1:
                both = dot_split(both, unpacked(tz_ref[p, slot + 1]))
            both = jnp.where(jnp.logical_and(upper, slot == here.z - 1), twice, both)
            high, low = halves(both)
            at = slice(HALF * slot, HALF * (slot + 1))
            for ref, part in ((pzh_ref, high), (pzl_ref, low)):
                ref[p, : 2 * NB, at] = part[:, :HALF]
                ref[p, 2 * NB :, at] = part[:, HALF:]
        both = dot_split(both, unpacked(tz_ref[p, 0]))
        tx_ref[p, here.x] = packed(both[NB:])
        for d in range(1, nx):
            along_x(tx_ref, p, d, sent_tx, received_tx).start()
        reach_ref[p] = jnp.where(here.z == 0, eye, both[:NB])

    def chain_x(p):
        arrived(next_ref.at[p], sent_n.at[p], received_n.at[p])
        ahead = unpacked(next_ref[p])
        ahead_high, ahead_low = halves(ahead)
        rhh_ref[p], rhl_ref[p] = ahead_high, ahead_low
        reh_ref[p, 8 * NB :], rel_ref[p, 8 * NB :] = halves(dot3(ahead_high, ahead_low, *halves(resp_ref[p])))
        await_x(tx_ref, p, sent_tx, received_tx)
        upto = jnp.zeros((NB, NB), F32)
        for slot in reversed(range(nx)):
            if slot < nx - 1:
                upto = dot_split(upto, unpacked(tx_ref[p, slot + 1]))
            upto = jnp.where(slot == here.x - 1, reach_ref[p], upto)
            high, low = halves(upto)
            at = slice(HALF * slot, HALF * (slot + 1))
            for ref, part in ((pxh_ref, high), (pxl_ref, low)):
                ref[p, :NB, at] = part[:, :HALF]
                ref[p, NB:, at] = part[:, HALF:]


    mine = eig_ref[...]
    turned = jnp.where(core == 0, mine, pltpu.roll(mine, NB, 1))
    turn_ref[0] = packed(turned[:, NB:])
    to_partner = remote(turn_ref.at[0], turned_ref.at[0], sent.at[0], received.at[0], here.partner)
    to_partner.start()

    def give(p, _):
        stored = order_ref[p]
        blocks_ref[y, p, :NB] = vt_ref[stored]
        blocks_ref[y, p, NB:] = packed(t_ref[stored])
        for d in (2, 1, 3):
            block_copy(p, d).start()
        return 0

    lax.fori_loop(0, sweeps, give, 0)
    rows_ref[...] = jnp.zeros_like(rows_ref)
    kept = turned[:, :NB]
    arrived(turned_ref.at[0], sent.at[0], received.at[0])
    got = unpacked(turned_ref[0])
    rows_ref[ABOVE : ABOVE + OWN] = jnp.concatenate(
        [jnp.where(core == 0, kept, got), jnp.where(core == 0, got, kept)], axis=0
    )
    edge_ref[sweeps] = packed(rows_ref[ABOVE : ABOVE + 2 * NB])
    edge_copy(sweeps).start()
    build(0)
    build(1)
    respond(0)
    build(2)
    respond(1)
    arrived(edges_ref.at[sweeps], sent_h.at[sweeps], received_h.at[sweeps])
    rows_ref[ABOVE + OWN : ABOVE + OWN + 2 * NB] = unpacked(edges_ref[sweeps])
    chain_z(0)

    index = lax.broadcasted_iota(jnp.int32, (10 * NB, NB), 0)

    def sweep(p, before):
        offset = offsets_ref[order_ref[p]]
        shift = offset - before
        window = rows_ref[pl.ds(NB + shift, 10 * NB), :]
        beyond = jnp.logical_and(here.last, index >= 9 * NB - offset)
        carried = jnp.logical_and(jnp.logical_not(here.first), jnp.logical_and(index >= NB, index < 2 * NB))
        inputs = jnp.where(jnp.logical_or(beyond, carried), 0.0, window)
        head = window[:NB]
        high, low = halves(inputs[NB : 7 * NB])
        end_a = dot3(mh_ref[0, p, 4 * NB :], ml_ref[0, p, 4 * NB :], high, low)
        second = jnp.concatenate([end_a, inputs[6 * NB :], jnp.zeros((NB, NB), F32)], axis=0)
        high_b, low_b = halves(second)
        end_b = dot3(mh_ref[1, p, 4 * NB :], ml_ref[1, p, 4 * NB :], high_b, low_b)
        sums_ref[p, here.z] = packed(end_b)
        for d in far:
            along_z(sums_ref, p, d, sent_z, received_z).start()
        body_a = dot3(mh_ref[0, p, : 4 * NB], ml_ref[0, p, : 4 * NB], high, low)
        edge_ref[p] = packed(body_a[: 2 * NB])
        edge_copy(p).start()
        rows_ref[NB:ABOVE] = head
        y_ref[: 4 * NB] = body_a
        y_ref[4 * NB : 8 * NB] = dot3(mh_ref[1, p, : 4 * NB], ml_ref[1, p, : 4 * NB], high_b, low_b)
        chain_x(p)
        y_ref[8 * NB :] = dot3(rhh_ref[p], rhl_ref[p], *halves(unpacked(sums_ref[p, here.z])))

        if p + 1 < sweeps:
            chain_z(p + 1)

        if p + 2 < sweeps:
            respond(p + 2)

        await_z(sums_ref, p, sent_z, received_z)
        high_z, low_z = halves(sums_ref[p].reshape(nz * HALF, 2 * NB))
        both = dot3(pzh_ref[p], pzl_ref[p], high_z, low_z)
        combined = both[: 2 * NB, :NB] + both[2 * NB :, NB:]
        totals_ref[p, here.x] = packed(combined[NB:])
        for d in range(1, nx):
            along_x(totals_ref, p, d, sent_x, received_x).start()
        arrived(edges_ref.at[p], sent_h.at[p], received_h.at[p])
        y_ref[8 * NB :] = y_ref[8 * NB :] + unpacked(edges_ref[p])

        if p + 3 < sweeps:
            build(p + 3)

        await_x(totals_ref, p, sent_x, received_x)
        high_x, low_x = halves(totals_ref[p].reshape(nx * HALF, 2 * NB))
        both = dot3(pxh_ref[p], pxl_ref[p], high_x, low_x)
        carry = combined[:NB] + both[:NB, :NB] + both[NB:, NB:]
        carry_high, carry_low = halves(carry)
        rows_ref[ABOVE : ABOVE + 10 * NB] = y_ref[...] + dot3(reh_ref[p], rel_ref[p], carry_high, carry_low)
        return offset

    last_offset = jnp.int32(0)
    for p in range(sweeps):
        last_offset = sweep(p, last_offset)


    ends_ref[0] = packed(rows_ref[ABOVE + 7 * NB : ABOVE + 8 * NB])
    to_next = remote(ends_ref.at[0], ends_ref.at[1], sent.at[1], received.at[1], here.following)
    to_next.start()

    def finish(p, _):
        for d in range(1, 4):
            block_copy(p, d).wait_send()
        map_copy(p).wait_send()
        head_copy(p).wait_send()
        edge_copy(p).wait_send()
        for d in range(1, nz):
            along_z(tz_ref, p, d, sent_tz, received_tz).wait_send()
            along_z(sums_ref, p, d, sent_z, received_z).wait_send()
        for d in range(1, nx):
            along_x(tx_ref, p, d, sent_tx, received_tx).wait_send()
            along_x(totals_ref, p, d, sent_x, received_x).wait_send()
        return 0

    lax.fori_loop(0, sweeps, finish, 0)
    edge_copy(sweeps).wait_send()
    to_partner.wait_send()
    arrived(ends_ref.at[1], sent.at[1], received.at[1])
    rows_ref[NB:ABOVE] = jnp.where(here.first, rows_ref[NB:ABOVE], unpacked(ends_ref[1]))
    final = rows_ref[pl.ds(ABOVE - last_offset, OWN), :]
    upper, lower = final[: 4 * NB], final[4 * NB :]
    turn_ref[1] = packed(jnp.where(core == 0, lower, upper))
    back = remote(turn_ref.at[1], turned_ref.at[1], sent.at[2], received.at[2], here.partner)
    back.start()
    kept = jnp.where(core == 0, upper, lower)
    arrived(turned_ref.at[1], sent.at[2], received.at[2])
    got = unpacked(turned_ref[1])
    out_ref[...] = beside(jnp.where(core == 0, kept, got), jnp.where(core == 0, got, kept))
    to_next.wait_send()
    back.wait_send()


def apply_sweeps(order, offsets, eigvecs, transposed, factors, nx, nz):
    sweeps = order.shape[0]
    dma = pltpu.SemaphoreType.DMA
    maps = (sweeps, 5 * NB, 6 * NB)
    full = (sweeps, NB, 2 * NB)
    scratch = [
        VM((4, sweeps, NB + HALF, 2 * NB), F32),
        VM(maps, F32),
        VM(maps, F32),
        VM((2,) + maps, BF16),
        VM((2,) + maps, BF16),
        VM((sweeps, NB, NB), F32),
        VM((sweeps, 10 * NB, NB), BF16),
        VM((sweeps, 10 * NB, NB), BF16),
        VM(full, F32),
        VM(full, F32),
        VM((sweeps, 2 * NB, NB), BF16),
        VM((sweeps, 2 * NB, NB), BF16),
        VM((sweeps, nz, HALF, 2 * NB), F32),
        VM((sweeps, nx, HALF, 2 * NB), F32),
        VM((sweeps, NB, NB), F32),
        VM((sweeps, 4 * NB, HALF * nz), BF16),
        VM((sweeps, 4 * NB, HALF * nz), BF16),
        VM((sweeps, 2 * NB, HALF * nx), BF16),
        VM((sweeps, 2 * NB, HALF * nx), BF16),
        VM((14 * NB, NB), F32),
        VM((2, 2 * NB, 2 * NB), F32),
        VM((2, 2 * NB, 2 * NB), F32),
        VM((sweeps + 1, NB, 2 * NB), F32),
        VM((sweeps + 1, NB, 2 * NB), F32),
        VM((sweeps, nz, HALF, 2 * NB), F32),
        VM((sweeps, nx, HALF, 2 * NB), F32),
        VM((2, HALF, 2 * NB), F32),
        VM((10 * NB, NB), F32),
        dma((sweeps, 4)),
        dma((sweeps, 4)),
        dma((sweeps,)),
        dma((sweeps,)),
        dma((sweeps,)),
        dma((sweeps,)),
        dma((sweeps, nz)),
        dma((sweeps, nz)),
        dma((sweeps, nx)),
        dma((sweeps, nx)),
        dma((3,)),
        dma((3,)),
        dma((sweeps, nz)),
        dma((sweeps, nz)),
        dma((sweeps, nx)),
        dma((sweeps, nx)),
        dma((sweeps + 1,)),
        dma((sweeps + 1,)),
    ]
    scalar, vector = pl.BlockSpec(memory_space=pltpu.SMEM), pl.BlockSpec(memory_space=VM)
    return pl.pallas_call(
        sweeps_kernel,
        out_shape=jax.ShapeDtypeStruct(eigvecs.shape, F32),
        in_specs=[scalar] * 2 + [vector] * 3,
        out_specs=vector,
        scratch_shapes=scratch,
        compiler_params=pltpu.CompilerParams(
            collective_id=0, has_side_effects=True, vmem_limit_bytes=60 * 1024 * 1024
        ),
        name="apply_sweeps",
    )(order, offsets, eigvecs, transposed, factors)


def solution(mesh):
    nz, cores, ny = 8, 2, mesh.shape["col"]
    nx = mesh.shape["row"] // (nz * cores)
    torus = Mesh(mesh.devices.reshape(nx, nz, cores, ny), ROW_COL)

    def local(eigvecs, reflectors, factors, order, offsets):
        transposed = jnp.swapaxes(reflectors[:, 0], 1, 2)
        return apply_sweeps(order, offsets, eigvecs, transposed, factors[:, 0], nx, nz)

    placed = (P(ROW, "y"), P(None, ROW_COL, None, None), P(None, ROW_COL, None, None), P(), P())
    return jax.shard_map(local, mesh=torus, in_specs=placed, out_specs=P(ROW, "y"), check_vma=False)
```

```python
import functools

import jax
import jax.numpy as jnp
from jax import lax
from jax.experimental import pallas as pl
from jax.experimental.pallas import tpu as pltpu
from jax.sharding import Mesh
from jax.sharding import PartitionSpec as P

ROW = ("x", "z", "core")
ROW_COL = ("x", "z", "core", "y")
MESH = pl.DeviceIdType.MESH
F32 = jnp.float32
BF16 = jnp.bfloat16
NB = 64
VM = pltpu.VMEM


def halves(a):
    high = a.astype(BF16)
    return high, (a - high.astype(F32)).astype(BF16)


def dot3(a_high, a_low, b_high, b_low):
    product = functools.partial(jnp.dot, preferred_element_type=F32)
    return product(a_high, b_high) + (product(a_high, b_low) + product(a_low, b_high))


def dot_split(a, b):
    return dot3(*halves(a), *halves(b))


def packed(a):
    n = a.shape[0] // 2
    return jnp.concatenate([a[:n], a[n:]], axis=1)


def unpacked(a):
    return jnp.concatenate([a[:, :NB], a[:, NB:]], axis=0)


def beside(a, b):
    return jnp.concatenate([a, b], axis=1)


def barrier(devices):
    semaphore = pltpu.get_barrier_semaphore()
    for device in devices:
        pl.semaphore_signal(semaphore, inc=1, device_id=device, device_id_type=MESH)
    pl.semaphore_wait(semaphore, len(devices))


def remote(source, target, sent, received, device):
    return pltpu.make_async_remote_copy(
        src_ref=source, dst_ref=target, send_sem=sent, recv_sem=received, device_id=device, device_id_type=MESH
    )


class Place:
    def __init__(self):
        self.nx, self.nz = lax.axis_size("x"), lax.axis_size("z")
        self.x, self.z, self.core = lax.axis_index("x"), lax.axis_index("z"), lax.axis_index("core")
        chips = self.nx * self.nz
        self.chip = self.x * self.nz + self.z
        following, before = lax.rem(self.chip + 1, chips), lax.rem(self.chip + chips - 1, chips)
        self.following = {"x": following // self.nz, "z": lax.rem(following, self.nz)}
        self.before = {"x": before // self.nz, "z": lax.rem(before, self.nz)}
        self.partner = {"core": 1 - self.core}
        self.first = self.chip == 0
        self.last = self.chip == chips - 1

    def z_peers(self):
        return [{"z": lax.rem(self.z + d, self.nz)} for d in range(1, self.nz)]

    def x_peers(self):
        return [{"x": lax.rem(self.x + d, self.nx)} for d in range(1, self.nx)]

    def y_peers(self):
        return [{"y": lax.rem(lax.axis_index("y") + d, 4)} for d in range(1, 4)]

    def greet(self):
        barrier([self.partner, self.following, self.before] + self.z_peers() + self.x_peers() + self.y_peers())


ABOVE = 2 * NB
OWN = 8 * NB
HALF = NB // 2


def sweeps_kernel(
    order_ref, offsets_ref, eig_ref, vt_ref, t_ref, out_ref,
    blocks_ref, own_ref, other_ref, mh_ref, ml_ref, resp_ref, reh_ref, rel_ref, head_ref, next_ref, rhh_ref, rhl_ref,
    tz_ref, tx_ref, reach_ref, pzh_ref, pzl_ref, pxh_ref, pxl_ref, eh_ref, el_ref,
    rows_ref, turn_ref, turned_ref, edge_ref, edges_ref, sums_ref, totals_ref, ends_ref, y_ref,
    sent_y, received_y, sent_m, received_m, sent_n, received_n, sent_tz, received_tz, sent_tx, received_tx,
    sent, received, sent_z, received_z, sent_x, received_x, sent_h, received_h,
):
    here = Place()
    nx, nz, core, y = here.nx, here.nz, here.core, lax.axis_index("y")
    sweeps = vt_ref.shape[0]
    far = sorted(range(1, nz), key=lambda d: -min(d, nz - d))
    here.greet()

    def arrived(target, send_sem, recv_sem):
        remote(target, target, send_sem, recv_sem, here.partner).wait_recv()


    def block_copy(p, d):
        at = blocks_ref.at[y, p]
        return remote(at, at, sent_y.at[p, d], received_y.at[p, y], {"y": lax.rem(y + d, 4)})

    def map_copy(p):
        return remote(own_ref.at[p], other_ref.at[p], sent_m.at[p], received_m.at[p], here.partner)

    def head_copy(p):
        return remote(head_ref.at[p], next_ref.at[p], sent_n.at[p], received_n.at[p], here.before)

    def along_z(ref, p, d, send_sems, recv_sems):
        at = ref.at[p, here.z]
        return remote(at, at, send_sems.at[p, d], recv_sems.at[p, here.z], {"z": lax.rem(here.z + d, nz)})

    def along_x(ref, p, d, send_sems, recv_sems):
        at = ref.at[p, here.x]
        return remote(at, at, send_sems.at[p, d], recv_sems.at[p, here.x], {"x": lax.rem(here.x + d, nx)})

    def edge_copy(p):
        return remote(edge_ref.at[p], edges_ref.at[p], sent_h.at[p], received_h.at[p], here.before)

    def await_z(ref, p, send_sems, recv_sems):
        for d in range(1, nz):
            slot = lax.rem(here.z + d, nz)
            arrived(ref.at[p, slot], send_sems.at[p, d], recv_sems.at[p, slot])

    def await_x(ref, p, send_sems, recv_sems):
        for d in range(1, nx):
            slot = lax.rem(here.x + d, nx)
            arrived(ref.at[p, slot], send_sems.at[p, d], recv_sems.at[p, slot])


    eye = (lax.broadcasted_iota(jnp.int32, (NB, NB), 0) == lax.broadcasted_iota(jnp.int32, (NB, NB), 1)).astype(F32)
    wide_eye = (
        lax.broadcasted_iota(jnp.int32, (2 * NB, 2 * NB), 0) == lax.broadcasted_iota(jnp.int32, (2 * NB, 2 * NB), 1)
    ).astype(F32)

    def give(p):
        stored = order_ref[p]
        blocks_ref[y, p, :NB] = vt_ref[stored]
        blocks_ref[y, p, NB:] = packed(t_ref[stored])
        for d in (2, 1, 3):
            block_copy(p, d).start()

    def build(p):
        for d in range(1, 4):
            slot = lax.rem(y + d, 4)
            arrived(blocks_ref.at[slot, p], sent_y.at[p, d], received_y.at[p, slot])
        if p + 1 < sweeps:
            give(p + 1)
        maps = []
        for j in range(4):
            vt = blocks_ref[j, p, :NB]
            t = unpacked(blocks_ref[j, p, NB:])
            vh, vl = halves(vt)
            wh, wl = halves(dot3(*halves(t), vh, vl))
            product = functools.partial(
                lax.dot_general, dimension_numbers=(((0,), (0,)), ((), ())), preferred_element_type=F32
            )
            maps.append(wide_eye - (product(vh, wh) + (product(vh, wl) + product(vl, wh))))
        carry = None
        for j in range(4):
            block = maps[j]
            rows = block if j == 0 else beside(dot_split(block[:, :NB], carry), block[:, NB:])
            done = jnp.concatenate([rows[:NB], jnp.zeros((NB, 6 * NB - rows.shape[1]), F32)], axis=1)
            own_ref[p, NB * j : NB * (j + 1), :] = done
            carry = rows[NB:]
        own_ref[p, 4 * NB :, :] = beside(carry, jnp.zeros((NB, NB), F32))
        map_copy(p).start()
        mh_ref[core, p], ml_ref[core, p] = halves(own_ref[p])

    def respond(p):
        arrived(other_ref.at[p], sent_m.at[p], received_m.at[p])
        mine_first, other_first = own_ref[p, :, : 2 * NB], other_ref[p, :, : 2 * NB]
        first = jnp.where(core == 0, mine_first, other_first)[:, :NB]
        second = jnp.where(core == 0, other_first, mine_first)[:, :NB]
        later = dot_split(second, first[4 * NB :])
        tz_ref[p, here.z] = packed(later[4 * NB :])
        for d in far:
            along_z(tz_ref, p, d, sent_tz, received_tz).start()
        head_ref[p] = packed(first[: 2 * NB])
        head_copy(p).start()
        resp_ref[p] = later[4 * NB :]
        mine_last, other_last = own_ref[p, 4 * NB :, :], other_ref[p, 4 * NB :, :]
        end_first = jnp.where(core == 0, mine_last, other_last)
        end_second = jnp.where(core == 0, other_last, mine_last)
        through = dot_split(end_second[:, :NB], end_first)
        eh_ref[p], el_ref[p] = halves(jnp.concatenate([through[:, : 5 * NB], end_second[:, NB : 5 * NB]], axis=1))
        reh_ref[p, : 4 * NB], rel_ref[p, : 4 * NB] = halves(first[: 4 * NB])
        reh_ref[p, 4 * NB : 8 * NB], rel_ref[p, 4 * NB : 8 * NB] = halves(later[: 4 * NB])
        mh_ref[1 - core, p], ml_ref[1 - core, p] = halves(other_ref[p])

    def chain_z(p):
        await_z(tz_ref, p, sent_tz, received_tz)
        both = jnp.concatenate([jnp.zeros((NB, NB), F32), eye], axis=0)
        upper = lax.broadcasted_iota(jnp.int32, (2 * NB, NB), 0) < NB
        twice = jnp.concatenate([eye, eye], axis=0)
        for slot in reversed(range(nz)):
            if slot < nz - 1:
                both = dot_split(both, unpacked(tz_ref[p, slot + 1]))
            both = jnp.where(jnp.logical_and(upper, slot == here.z - 1), twice, both)
            high, low = halves(both)
            at = slice(HALF * slot, HALF * (slot + 1))
            for ref, part in ((pzh_ref, high), (pzl_ref, low)):
                ref[p, : 2 * NB, at] = part[:, :HALF]
                ref[p, 2 * NB :, at] = part[:, HALF:]
        both = dot_split(both, unpacked(tz_ref[p, 0]))
        tx_ref[p, here.x] = packed(both[NB:])
        for d in range(1, nx):
            along_x(tx_ref, p, d, sent_tx, received_tx).start()
        reach_ref[p] = jnp.where(here.z == 0, eye, both[:NB])

    def chain_x(p):
        arrived(next_ref.at[p], sent_n.at[p], received_n.at[p])
        ahead = unpacked(next_ref[p])
        ahead_high, ahead_low = halves(ahead)
        rhh_ref[p], rhl_ref[p] = ahead_high, ahead_low
        reh_ref[p, 8 * NB :], rel_ref[p, 8 * NB :] = halves(dot3(ahead_high, ahead_low, *halves(resp_ref[p])))
        await_x(tx_ref, p, sent_tx, received_tx)
        upto = jnp.zeros((NB, NB), F32)
        for slot in reversed(range(nx)):
            if slot < nx - 1:
                upto = dot_split(upto, unpacked(tx_ref[p, slot + 1]))
            upto = jnp.where(slot == here.x - 1, reach_ref[p], upto)
            high, low = halves(upto)
            at = slice(HALF * slot, HALF * (slot + 1))
            for ref, part in ((pxh_ref, high), (pxl_ref, low)):
                ref[p, :NB, at] = part[:, :HALF]
                ref[p, NB:, at] = part[:, HALF:]


    give(0)
    mine = eig_ref[...]
    turned = jnp.where(core == 0, mine, pltpu.roll(mine, NB, 1))
    turn_ref[0] = packed(turned[:, NB:])
    to_partner = remote(turn_ref.at[0], turned_ref.at[0], sent.at[0], received.at[0], here.partner)
    to_partner.start()

    rows_ref[...] = jnp.zeros_like(rows_ref)
    kept = turned[:, :NB]
    arrived(turned_ref.at[0], sent.at[0], received.at[0])
    got = unpacked(turned_ref[0])
    rows_ref[ABOVE : ABOVE + OWN] = jnp.concatenate(
        [jnp.where(core == 0, kept, got), jnp.where(core == 0, got, kept)], axis=0
    )
    edge_ref[sweeps] = packed(rows_ref[ABOVE : ABOVE + 2 * NB])
    edge_copy(sweeps).start()
    build(0)
    respond(0)
    arrived(edges_ref.at[sweeps], sent_h.at[sweeps], received_h.at[sweeps])
    rows_ref[ABOVE + OWN : ABOVE + OWN + 2 * NB] = unpacked(edges_ref[sweeps])

    index = lax.broadcasted_iota(jnp.int32, (10 * NB, NB), 0)

    def sweep(p, before):
        offset = offsets_ref[order_ref[p]]
        shift = offset - before
        window = rows_ref[pl.ds(NB + shift, 10 * NB), :]
        beyond = jnp.logical_and(here.last, index >= 9 * NB - offset)
        carried = jnp.logical_and(jnp.logical_not(here.first), jnp.logical_and(index >= NB, index < 2 * NB))
        inputs = jnp.where(jnp.logical_or(beyond, carried), 0.0, window)
        head = window[:NB]
        high, low = halves(inputs[NB:])
        sums_ref[p, here.z] = packed(dot3(eh_ref[p], el_ref[p], high, low))
        for d in far:
            along_z(sums_ref, p, d, sent_z, received_z).start()
        high_a, low_a = high[: 6 * NB], low[: 6 * NB]
        body_a = dot3(mh_ref[0, p, : 4 * NB], ml_ref[0, p, : 4 * NB], high_a, low_a)
        edge_ref[p] = packed(body_a[: 2 * NB])
        edge_copy(p).start()
        rows_ref[NB:ABOVE] = head
        y_ref[: 4 * NB] = body_a
        end_a = dot3(mh_ref[0, p, 4 * NB :], ml_ref[0, p, 4 * NB :], high_a, low_a)
        second = jnp.concatenate([end_a, inputs[6 * NB :], jnp.zeros((NB, NB), F32)], axis=0)
        y_ref[4 * NB : 8 * NB] = dot3(mh_ref[1, p, : 4 * NB], ml_ref[1, p, : 4 * NB], *halves(second))
        if p == 0:
            build(1)
        chain_z(p)
        if p + 1 < sweeps:
            respond(p + 1)

        await_z(sums_ref, p, sent_z, received_z)
        high_z, low_z = halves(sums_ref[p].reshape(nz * HALF, 2 * NB))
        both = dot3(pzh_ref[p], pzl_ref[p], high_z, low_z)
        combined = both[: 2 * NB, :NB] + both[2 * NB :, NB:]
        totals_ref[p, here.x] = packed(combined[NB:])
        for d in sorted(range(1, nx), key=lambda d: -min(d, nx - d)):
            along_x(totals_ref, p, d, sent_x, received_x).start()
        if p + 2 < sweeps:
            build(p + 2)
        chain_x(p)
        ahead = dot3(rhh_ref[p], rhl_ref[p], *halves(unpacked(sums_ref[p, here.z])))
        arrived(edges_ref.at[p], sent_h.at[p], received_h.at[p])
        y_ref[8 * NB :] = unpacked(edges_ref[p]) + ahead

        await_x(totals_ref, p, sent_x, received_x)
        high_x, low_x = halves(totals_ref[p].reshape(nx * HALF, 2 * NB))
        both = dot3(pxh_ref[p], pxl_ref[p], high_x, low_x)
        carry = combined[:NB] + both[:NB, :NB] + both[NB:, NB:]
        carry_high, carry_low = halves(carry)
        rows_ref[ABOVE : ABOVE + 10 * NB] = y_ref[...] + dot3(reh_ref[p], rel_ref[p], carry_high, carry_low)
        return offset

    last_offset = jnp.int32(0)
    for p in range(sweeps):
        last_offset = sweep(p, last_offset)


    ends_ref[0] = packed(rows_ref[ABOVE + 7 * NB : ABOVE + 8 * NB])
    to_next = remote(ends_ref.at[0], ends_ref.at[1], sent.at[1], received.at[1], here.following)
    to_next.start()

    def finish(p, _):
        for d in range(1, 4):
            block_copy(p, d).wait_send()
        map_copy(p).wait_send()
        head_copy(p).wait_send()
        edge_copy(p).wait_send()
        for d in range(1, nz):
            along_z(tz_ref, p, d, sent_tz, received_tz).wait_send()
            along_z(sums_ref, p, d, sent_z, received_z).wait_send()
        for d in range(1, nx):
            along_x(tx_ref, p, d, sent_tx, received_tx).wait_send()
            along_x(totals_ref, p, d, sent_x, received_x).wait_send()
        return 0

    lax.fori_loop(0, sweeps, finish, 0)
    edge_copy(sweeps).wait_send()
    to_partner.wait_send()
    arrived(ends_ref.at[1], sent.at[1], received.at[1])
    rows_ref[NB:ABOVE] = jnp.where(here.first, rows_ref[NB:ABOVE], unpacked(ends_ref[1]))
    final = rows_ref[pl.ds(ABOVE - last_offset, OWN), :]
    upper, lower = final[: 4 * NB], final[4 * NB :]
    turn_ref[1] = packed(jnp.where(core == 0, lower, upper))
    back = remote(turn_ref.at[1], turned_ref.at[1], sent.at[2], received.at[2], here.partner)
    back.start()
    kept = jnp.where(core == 0, upper, lower)
    arrived(turned_ref.at[1], sent.at[2], received.at[2])
    got = unpacked(turned_ref[1])
    out_ref[...] = beside(jnp.where(core == 0, kept, got), jnp.where(core == 0, got, kept))
    to_next.wait_send()
    back.wait_send()


def apply_sweeps(order, offsets, eigvecs, transposed, factors, nx, nz):
    sweeps = order.shape[0]
    dma = pltpu.SemaphoreType.DMA
    maps = (sweeps, 5 * NB, 6 * NB)
    full = (sweeps, NB, 2 * NB)
    scratch = [
        VM((4, sweeps, NB + HALF, 2 * NB), F32),
        VM(maps, F32),
        VM(maps, F32),
        VM((2,) + maps, BF16),
        VM((2,) + maps, BF16),
        VM((sweeps, NB, NB), F32),
        VM((sweeps, 10 * NB, NB), BF16),
        VM((sweeps, 10 * NB, NB), BF16),
        VM(full, F32),
        VM(full, F32),
        VM((sweeps, 2 * NB, NB), BF16),
        VM((sweeps, 2 * NB, NB), BF16),
        VM((sweeps, nz, HALF, 2 * NB), F32),
        VM((sweeps, nx, HALF, 2 * NB), F32),
        VM((sweeps, NB, NB), F32),
        VM((sweeps, 4 * NB, HALF * nz), BF16),
        VM((sweeps, 4 * NB, HALF * nz), BF16),
        VM((sweeps, 2 * NB, HALF * nx), BF16),
        VM((sweeps, 2 * NB, HALF * nx), BF16),
        VM((sweeps, NB, 9 * NB), BF16),
        VM((sweeps, NB, 9 * NB), BF16),
        VM((14 * NB, NB), F32),
        VM((2, 2 * NB, 2 * NB), F32),
        VM((2, 2 * NB, 2 * NB), F32),
        VM((sweeps + 1, NB, 2 * NB), F32),
        VM((sweeps + 1, NB, 2 * NB), F32),
        VM((sweeps, nz, HALF, 2 * NB), F32),
        VM((sweeps, nx, HALF, 2 * NB), F32),
        VM((2, HALF, 2 * NB), F32),
        VM((10 * NB, NB), F32),
        dma((sweeps, 4)),
        dma((sweeps, 4)),
        dma((sweeps,)),
        dma((sweeps,)),
        dma((sweeps,)),
        dma((sweeps,)),
        dma((sweeps, nz)),
        dma((sweeps, nz)),
        dma((sweeps, nx)),
        dma((sweeps, nx)),
        dma((3,)),
        dma((3,)),
        dma((sweeps, nz)),
        dma((sweeps, nz)),
        dma((sweeps, nx)),
        dma((sweeps, nx)),
        dma((sweeps + 1,)),
        dma((sweeps + 1,)),
    ]
    scalar, vector = pl.BlockSpec(memory_space=pltpu.SMEM), pl.BlockSpec(memory_space=VM)
    return pl.pallas_call(
        sweeps_kernel,
        out_shape=jax.ShapeDtypeStruct(eigvecs.shape, F32),
        in_specs=[scalar] * 2 + [vector] * 3,
        out_specs=vector,
        scratch_shapes=scratch,
        compiler_params=pltpu.CompilerParams(
            collective_id=0, has_side_effects=True, vmem_limit_bytes=60 * 1024 * 1024
        ),
        name="apply_sweeps",
    )(order, offsets, eigvecs, transposed, factors)


def solution(mesh):
    nz, cores, ny = 8, 2, mesh.shape["col"]
    nx = mesh.shape["row"] // (nz * cores)
    torus = Mesh(mesh.devices.reshape(nx, nz, cores, ny), ROW_COL)

    def local(eigvecs, reflectors, factors, order, offsets):
        transposed = jnp.swapaxes(reflectors[:, 0], 1, 2)
        return apply_sweeps(order, offsets, eigvecs, transposed, factors[:, 0], nx, nz)

    placed = (P(ROW, "y"), P(None, ROW_COL, None, None), P(None, ROW_COL, None, None), P(), P())
    return jax.shard_map(local, mesh=torus, in_specs=placed, out_specs=P(ROW, "y"), check_vma=False)
```

```python
import functools

import jax
import jax.numpy as jnp
from jax import lax
from jax.experimental import pallas as pl
from jax.experimental.pallas import tpu as pltpu
from jax.sharding import Mesh
from jax.sharding import PartitionSpec as P

ROW = ("x", "z", "core")
ROW_COL = ("x", "z", "core", "y")
MESH = pl.DeviceIdType.MESH
F32 = jnp.float32
BF16 = jnp.bfloat16
NB = 64
VM = pltpu.VMEM


def halves(a):
    high = a.astype(BF16)
    return high, (a - high.astype(F32)).astype(BF16)


def dot3(a_high, a_low, b_high, b_low):
    product = functools.partial(jnp.dot, preferred_element_type=F32)
    return product(a_high, b_high) + (product(a_high, b_low) + product(a_low, b_high))


def dot_split(a, b):
    return dot3(*halves(a), *halves(b))


def three_terms(a):
    high, low = halves(a)
    return jnp.concatenate([high, high, low], axis=1)


def three_below(a):
    high, low = halves(a)
    return jnp.concatenate([high, low, high], axis=0)


def packed(a):
    n = a.shape[0] // 2
    return jnp.concatenate([a[:n], a[n:]], axis=1)


def unpacked(a):
    return jnp.concatenate([a[:, :NB], a[:, NB:]], axis=0)


def beside(a, b):
    return jnp.concatenate([a, b], axis=1)


def barrier(devices):
    semaphore = pltpu.get_barrier_semaphore()
    for device in devices:
        pl.semaphore_signal(semaphore, inc=1, device_id=device, device_id_type=MESH)
    pl.semaphore_wait(semaphore, len(devices))


def remote(source, target, sent, received, device):
    return pltpu.make_async_remote_copy(
        src_ref=source, dst_ref=target, send_sem=sent, recv_sem=received, device_id=device, device_id_type=MESH
    )


class Place:
    def __init__(self):
        self.nx, self.nz = lax.axis_size("x"), lax.axis_size("z")
        self.x, self.z, self.core = lax.axis_index("x"), lax.axis_index("z"), lax.axis_index("core")
        chips = self.nx * self.nz
        self.chip = self.x * self.nz + self.z
        following, before = lax.rem(self.chip + 1, chips), lax.rem(self.chip + chips - 1, chips)
        self.following = {"x": following // self.nz, "z": lax.rem(following, self.nz)}
        self.before = {"x": before // self.nz, "z": lax.rem(before, self.nz)}
        self.partner = {"core": 1 - self.core}
        self.first = self.chip == 0
        self.last = self.chip == chips - 1

    def z_peers(self):
        return [{"z": lax.rem(self.z + d, self.nz)} for d in range(1, self.nz)]

    def x_peers(self):
        return [{"x": lax.rem(self.x + d, self.nx)} for d in range(1, self.nx)]

    def y_peers(self):
        return [{"y": lax.rem(lax.axis_index("y") + d, 4)} for d in range(1, 4)]

    def greet(self):
        barrier([self.partner, self.following, self.before] + self.z_peers() + self.x_peers() + self.y_peers())


ABOVE = 2 * NB
OWN = 8 * NB
HALF = NB // 2


def sweeps_kernel(
    order_ref, offsets_ref, eig_ref, vt_ref, t_ref, out_ref,
    blocks_ref, own_ref, other_ref, mh_ref, ml_ref, resp_ref, re_ref, head_ref, next_ref,
    tz_ref, tx_ref, reach_ref, pzh_ref, pzl_ref, pxh_ref, pxl_ref, eh_ref, el_ref,
    rows_ref, turn_ref, turned_ref, edge_ref, edges_ref, sums_ref, totals_ref, ends_ref, y_ref,
    sent_y, received_y, sent_m, received_m, sent_n, received_n, sent_tz, received_tz, sent_tx, received_tx,
    sent, received, sent_z, received_z, sent_x, received_x, sent_h, received_h,
):
    here = Place()
    nx, nz, core, y = here.nx, here.nz, here.core, lax.axis_index("y")
    sweeps = vt_ref.shape[0]
    far = sorted(range(1, nz), key=lambda d: -min(d, nz - d))
    here.greet()

    def arrived(target, send_sem, recv_sem):
        remote(target, target, send_sem, recv_sem, here.partner).wait_recv()


    def block_copy(p, d):
        at = blocks_ref.at[y, p]
        return remote(at, at, sent_y.at[p, d], received_y.at[p, y], {"y": lax.rem(y + d, 4)})

    def map_copy(p):
        return remote(own_ref.at[p], other_ref.at[p], sent_m.at[p], received_m.at[p], here.partner)

    def head_copy(p):
        return remote(head_ref.at[p], next_ref.at[p], sent_n.at[p], received_n.at[p], here.before)

    def along_z(ref, p, d, send_sems, recv_sems):
        at = ref.at[p, here.z]
        return remote(at, at, send_sems.at[p, d], recv_sems.at[p, here.z], {"z": lax.rem(here.z + d, nz)})

    def along_x(ref, p, d, send_sems, recv_sems):
        at = ref.at[p, here.x]
        return remote(at, at, send_sems.at[p, d], recv_sems.at[p, here.x], {"x": lax.rem(here.x + d, nx)})

    def edge_copy(p):
        return remote(edge_ref.at[p], edges_ref.at[p], sent_h.at[p], received_h.at[p], here.before)

    def await_z(ref, p, send_sems, recv_sems):
        for d in range(1, nz):
            slot = lax.rem(here.z + d, nz)
            arrived(ref.at[p, slot], send_sems.at[p, d], recv_sems.at[p, slot])

    def await_x(ref, p, send_sems, recv_sems):
        for d in range(1, nx):
            slot = lax.rem(here.x + d, nx)
            arrived(ref.at[p, slot], send_sems.at[p, d], recv_sems.at[p, slot])


    eye = (lax.broadcasted_iota(jnp.int32, (NB, NB), 0) == lax.broadcasted_iota(jnp.int32, (NB, NB), 1)).astype(F32)
    wide_eye = (
        lax.broadcasted_iota(jnp.int32, (2 * NB, 2 * NB), 0) == lax.broadcasted_iota(jnp.int32, (2 * NB, 2 * NB), 1)
    ).astype(F32)

    def give(p):
        stored = order_ref[p]
        blocks_ref[y, p, :NB] = vt_ref[stored]
        blocks_ref[y, p, NB:] = packed(t_ref[stored])
        for d in (2, 1, 3):
            block_copy(p, d).start()

    def build(p):
        for d in range(1, 4):
            slot = lax.rem(y + d, 4)
            arrived(blocks_ref.at[slot, p], sent_y.at[p, d], received_y.at[p, slot])
        if p + 1 < sweeps:
            give(p + 1)
        maps = []
        for j in range(4):
            vt = blocks_ref[j, p, :NB]
            t = unpacked(blocks_ref[j, p, NB:])
            vh, vl = halves(vt)
            w = dot3(*halves(t), vh, vl)
            left = jnp.concatenate([vh, vh, vl], axis=0)
            product = lax.dot_general(
                left, three_below(w), (((0,), (0,)), ((), ())), preferred_element_type=F32
            )
            maps.append(wide_eye - product)
        carry = None
        for j in range(4):
            block = maps[j]
            rows = block if j == 0 else beside(dot_split(block[:, :NB], carry), block[:, NB:])
            done = jnp.concatenate([rows[:NB], jnp.zeros((NB, 6 * NB - rows.shape[1]), F32)], axis=1)
            own_ref[p, NB * j : NB * (j + 1), :] = done
            carry = rows[NB:]
        own_ref[p, 4 * NB :, :] = beside(carry, jnp.zeros((NB, NB), F32))
        map_copy(p).start()

    def respond(p):
        arrived(other_ref.at[p], sent_m.at[p], received_m.at[p])
        mine_first, other_first = own_ref[p, :, : 2 * NB], other_ref[p, :, : 2 * NB]
        first = jnp.where(core == 0, mine_first, other_first)[:, :NB]
        second = jnp.where(core == 0, other_first, mine_first)[:, :NB]
        later = dot_split(second, first[4 * NB :])
        tz_ref[p, here.z] = packed(later[4 * NB :])
        for d in far:
            along_z(tz_ref, p, d, sent_tz, received_tz).start()
        head_ref[p] = packed(first[: 2 * NB])
        head_copy(p).start()
        resp_ref[p] = later[4 * NB :]
        mine_last, other_last = own_ref[p, 4 * NB :, :], other_ref[p, 4 * NB :, :]
        end_first = jnp.where(core == 0, mine_last, other_last)
        end_second = jnp.where(core == 0, other_last, mine_last)
        through = dot_split(end_second[:, :NB], end_first)
        eh_ref[p], el_ref[p] = halves(jnp.concatenate([through[:, : 5 * NB], end_second[:, NB : 5 * NB]], axis=1))
        re_ref[p, : 4 * NB] = three_terms(first[: 4 * NB])
        re_ref[p, 4 * NB : 8 * NB] = three_terms(later[: 4 * NB])
        mh_ref[1 - core, p], ml_ref[1 - core, p] = halves(other_ref[p])
        mh_ref[core, p], ml_ref[core, p] = halves(own_ref[p])

    def chain_z(p):
        await_z(tz_ref, p, sent_tz, received_tz)
        both = jnp.concatenate([jnp.zeros((NB, NB), F32), eye], axis=0)
        upper = lax.broadcasted_iota(jnp.int32, (2 * NB, NB), 0) < NB
        twice = jnp.concatenate([eye, eye], axis=0)
        for slot in reversed(range(nz)):
            if slot < nz - 1:
                both = dot_split(both, unpacked(tz_ref[p, slot + 1]))
            both = jnp.where(jnp.logical_and(upper, slot == here.z - 1), twice, both)
            high, low = halves(both)
            at = slice(HALF * slot, HALF * (slot + 1))
            for ref, part in ((pzh_ref, high), (pzl_ref, low)):
                ref[p, :NB, at] = part[NB:, :HALF]
                ref[p, NB : 2 * NB, at] = part[NB:, HALF:]
                ref[p, 2 * NB : 3 * NB, at] = part[:NB, :HALF]
                ref[p, 3 * NB :, at] = part[:NB, HALF:]
        both = dot_split(both, unpacked(tz_ref[p, 0]))
        tx_ref[p, here.x] = packed(both[NB:])
        for d in range(1, nx):
            along_x(tx_ref, p, d, sent_tx, received_tx).start()
        reach_ref[p] = jnp.where(here.z == 0, eye, both[:NB])

    def ahead_of(p):
        arrived(next_ref.at[p], sent_n.at[p], received_n.at[p])
        ahead = unpacked(next_ref[p])
        ahead_high, ahead_low = halves(ahead)
        re_ref[p, 8 * NB :] = three_terms(dot3(ahead_high, ahead_low, *halves(resp_ref[p])))
        y_ref[8 * NB :] = dot3(ahead_high, ahead_low, *halves(unpacked(sums_ref[p, here.z])))

    def chain_x(p):
        await_x(tx_ref, p, sent_tx, received_tx)
        upto = jnp.zeros((NB, NB), F32)
        for slot in reversed(range(nx)):
            if slot < nx - 1:
                upto = dot_split(upto, unpacked(tx_ref[p, slot + 1]))
            upto = jnp.where(slot == here.x - 1, reach_ref[p], upto)
            high, low = halves(upto)
            at = slice(HALF * slot, HALF * (slot + 1))
            for ref, part in ((pxh_ref, high), (pxl_ref, low)):
                ref[p, :NB, at] = part[:, :HALF]
                ref[p, NB:, at] = part[:, HALF:]


    give(0)
    mine = eig_ref[...]
    turned = jnp.where(core == 0, mine, pltpu.roll(mine, NB, 1))
    turn_ref[0] = packed(turned[:, NB:])
    to_partner = remote(turn_ref.at[0], turned_ref.at[0], sent.at[0], received.at[0], here.partner)
    to_partner.start()

    rows_ref[...] = jnp.zeros_like(rows_ref)
    kept = turned[:, :NB]
    arrived(turned_ref.at[0], sent.at[0], received.at[0])
    got = unpacked(turned_ref[0])
    rows_ref[ABOVE : ABOVE + OWN] = jnp.concatenate(
        [jnp.where(core == 0, kept, got), jnp.where(core == 0, got, kept)], axis=0
    )
    edge_ref[sweeps] = packed(rows_ref[ABOVE : ABOVE + 2 * NB])
    edge_copy(sweeps).start()
    build(0)
    respond(0)
    arrived(edges_ref.at[sweeps], sent_h.at[sweeps], received_h.at[sweeps])
    rows_ref[ABOVE + OWN : ABOVE + OWN + 2 * NB] = unpacked(edges_ref[sweeps])

    index = lax.broadcasted_iota(jnp.int32, (10 * NB, NB), 0)

    def sweep(p, before):
        offset = offsets_ref[order_ref[p]]
        shift = offset - before
        window = rows_ref[pl.ds(NB + shift, 10 * NB), :]
        beyond = jnp.logical_and(here.last, index >= 9 * NB - offset)
        carried = jnp.logical_and(jnp.logical_not(here.first), jnp.logical_and(index >= NB, index < 2 * NB))
        inputs = jnp.where(jnp.logical_or(beyond, carried), 0.0, window)
        head = window[:NB]
        high, low = halves(inputs[NB:])
        sums_ref[p, here.z] = packed(dot3(eh_ref[p], el_ref[p], high, low))
        for d in far:
            along_z(sums_ref, p, d, sent_z, received_z).start()
        high_a, low_a = high[: 6 * NB], low[: 6 * NB]
        body_a = dot3(mh_ref[0, p, : 4 * NB], ml_ref[0, p, : 4 * NB], high_a, low_a)
        edge_ref[p] = packed(body_a[: 2 * NB])
        edge_copy(p).start()
        rows_ref[NB:ABOVE] = head
        y_ref[: 4 * NB] = body_a
        end_a = dot3(mh_ref[0, p, 4 * NB :], ml_ref[0, p, 4 * NB :], high_a, low_a)
        second = jnp.concatenate([end_a, inputs[6 * NB :], jnp.zeros((NB, NB), F32)], axis=0)
        y_ref[4 * NB : 8 * NB] = dot3(mh_ref[1, p, : 4 * NB], ml_ref[1, p, : 4 * NB], *halves(second))
        if p == 0:
            build(1)
        chain_z(p)
        if p + 1 < sweeps:
            respond(p + 1)
        ahead_of(p)

        await_z(sums_ref, p, sent_z, received_z)
        high_z, low_z = halves(sums_ref[p].reshape(nz * HALF, 2 * NB))
        both = dot3(pzh_ref[p, : 2 * NB], pzl_ref[p, : 2 * NB], high_z, low_z)
        totals_ref[p, here.x] = packed(both[:NB, :NB] + both[NB:, NB:])
        for d in sorted(range(1, nx), key=lambda d: -min(d, nx - d)):
            along_x(totals_ref, p, d, sent_x, received_x).start()
        both = dot3(pzh_ref[p, 2 * NB :], pzl_ref[p, 2 * NB :], high_z, low_z)
        near = both[:NB, :NB] + both[NB:, NB:]
        if p + 2 < sweeps:
            build(p + 2)
        chain_x(p)
        arrived(edges_ref.at[p], sent_h.at[p], received_h.at[p])
        y_ref[8 * NB :] = unpacked(edges_ref[p]) + y_ref[8 * NB :]

        await_x(totals_ref, p, sent_x, received_x)
        high_x, low_x = halves(totals_ref[p].reshape(nx * HALF, 2 * NB))
        both = dot3(pxh_ref[p], pxl_ref[p], high_x, low_x)
        carry = near + both[:NB, :NB] + both[NB:, NB:]
        rows_ref[ABOVE : ABOVE + 10 * NB] = y_ref[...] + jnp.dot(
            re_ref[p], three_below(carry), preferred_element_type=F32
        )
        return offset

    last_offset = jnp.int32(0)
    for p in range(sweeps):
        last_offset = sweep(p, last_offset)


    ends_ref[0] = packed(rows_ref[ABOVE + 7 * NB : ABOVE + 8 * NB])
    to_next = remote(ends_ref.at[0], ends_ref.at[1], sent.at[1], received.at[1], here.following)
    to_next.start()

    def finish(p, _):
        for d in range(1, 4):
            block_copy(p, d).wait_send()
        map_copy(p).wait_send()
        head_copy(p).wait_send()
        edge_copy(p).wait_send()
        for d in range(1, nz):
            along_z(tz_ref, p, d, sent_tz, received_tz).wait_send()
            along_z(sums_ref, p, d, sent_z, received_z).wait_send()
        for d in range(1, nx):
            along_x(tx_ref, p, d, sent_tx, received_tx).wait_send()
            along_x(totals_ref, p, d, sent_x, received_x).wait_send()
        return 0

    lax.fori_loop(0, sweeps, finish, 0)
    edge_copy(sweeps).wait_send()
    to_partner.wait_send()
    arrived(ends_ref.at[1], sent.at[1], received.at[1])
    rows_ref[NB:ABOVE] = jnp.where(here.first, rows_ref[NB:ABOVE], unpacked(ends_ref[1]))
    final = rows_ref[pl.ds(ABOVE - last_offset, OWN), :]
    upper, lower = final[: 4 * NB], final[4 * NB :]
    turn_ref[1] = packed(jnp.where(core == 0, lower, upper))
    back = remote(turn_ref.at[1], turned_ref.at[1], sent.at[2], received.at[2], here.partner)
    back.start()
    kept = jnp.where(core == 0, upper, lower)
    arrived(turned_ref.at[1], sent.at[2], received.at[2])
    got = unpacked(turned_ref[1])
    out_ref[...] = beside(jnp.where(core == 0, kept, got), jnp.where(core == 0, got, kept))
    to_next.wait_send()
    back.wait_send()


def apply_sweeps(order, offsets, eigvecs, transposed, factors, nx, nz):
    sweeps = order.shape[0]
    dma = pltpu.SemaphoreType.DMA
    maps = (sweeps, 5 * NB, 6 * NB)
    full = (sweeps, NB, 2 * NB)
    scratch = [
        VM((4, sweeps, NB + HALF, 2 * NB), F32),
        VM(maps, F32),
        VM(maps, F32),
        VM((2,) + maps, BF16),
        VM((2,) + maps, BF16),
        VM((sweeps, NB, NB), F32),
        VM((sweeps, 10 * NB, 3 * NB), BF16),
        VM(full, F32),
        VM(full, F32),
        VM((sweeps, nz, HALF, 2 * NB), F32),
        VM((sweeps, nx, HALF, 2 * NB), F32),
        VM((sweeps, NB, NB), F32),
        VM((sweeps, 4 * NB, HALF * nz), BF16),
        VM((sweeps, 4 * NB, HALF * nz), BF16),
        VM((sweeps, 2 * NB, HALF * nx), BF16),
        VM((sweeps, 2 * NB, HALF * nx), BF16),
        VM((sweeps, NB, 9 * NB), BF16),
        VM((sweeps, NB, 9 * NB), BF16),
        VM((14 * NB, NB), F32),
        VM((2, 2 * NB, 2 * NB), F32),
        VM((2, 2 * NB, 2 * NB), F32),
        VM((sweeps + 1, NB, 2 * NB), F32),
        VM((sweeps + 1, NB, 2 * NB), F32),
        VM((sweeps, nz, HALF, 2 * NB), F32),
        VM((sweeps, nx, HALF, 2 * NB), F32),
        VM((2, HALF, 2 * NB), F32),
        VM((10 * NB, NB), F32),
        dma((sweeps, 4)),
        dma((sweeps, 4)),
        dma((sweeps,)),
        dma((sweeps,)),
        dma((sweeps,)),
        dma((sweeps,)),
        dma((sweeps, nz)),
        dma((sweeps, nz)),
        dma((sweeps, nx)),
        dma((sweeps, nx)),
        dma((3,)),
        dma((3,)),
        dma((sweeps, nz)),
        dma((sweeps, nz)),
        dma((sweeps, nx)),
        dma((sweeps, nx)),
        dma((sweeps + 1,)),
        dma((sweeps + 1,)),
    ]
    scalar, vector = pl.BlockSpec(memory_space=pltpu.SMEM), pl.BlockSpec(memory_space=VM)
    return pl.pallas_call(
        sweeps_kernel,
        out_shape=jax.ShapeDtypeStruct(eigvecs.shape, F32),
        in_specs=[scalar] * 2 + [vector] * 3,
        out_specs=vector,
        scratch_shapes=scratch,
        compiler_params=pltpu.CompilerParams(
            collective_id=0, has_side_effects=True, vmem_limit_bytes=60 * 1024 * 1024
        ),
        name="apply_sweeps",
    )(order, offsets, eigvecs, transposed, factors)


def solution(mesh):
    nz, cores, ny = 8, 2, mesh.shape["col"]
    nx = mesh.shape["row"] // (nz * cores)
    torus = Mesh(mesh.devices.reshape(nx, nz, cores, ny), ROW_COL)

    def local(eigvecs, reflectors, factors, order, offsets):
        transposed = jnp.swapaxes(reflectors[:, 0], 1, 2)
        return apply_sweeps(order, offsets, eigvecs, transposed, factors[:, 0], nx, nz)

    placed = (P(ROW, "y"), P(None, ROW_COL, None, None), P(None, ROW_COL, None, None), P(), P())
    return jax.shard_map(local, mesh=torus, in_specs=placed, out_specs=P(ROW, "y"), check_vma=False)
```

```python
import functools

import jax
import jax.numpy as jnp
from jax import lax
from jax.experimental import pallas as pl
from jax.experimental.pallas import tpu as pltpu
from jax.sharding import Mesh
from jax.sharding import PartitionSpec as P

ROW = ("x", "z", "core")
ROW_COL = ("x", "z", "core", "y")
MESH = pl.DeviceIdType.MESH
F32 = jnp.float32
BF16 = jnp.bfloat16
NB = 64
VM = pltpu.VMEM


def halves(a):
    high = a.astype(BF16)
    return high, (a - high.astype(F32)).astype(BF16)


def dot3(a_high, a_low, b_high, b_low):
    product = functools.partial(jnp.dot, preferred_element_type=F32)
    return product(a_high, b_high) + (product(a_high, b_low) + product(a_low, b_high))


def dot_split(a, b):
    return dot3(*halves(a), *halves(b))


def three_terms(a):
    high, low = halves(a)
    return jnp.concatenate([high, high, low], axis=1)


def three_below(a):
    high, low = halves(a)
    return jnp.concatenate([high, low, high], axis=0)


def packed(a):
    n = a.shape[0] // 2
    return jnp.concatenate([a[:n], a[n:]], axis=1)


def unpacked(a):
    return jnp.concatenate([a[:, :NB], a[:, NB:]], axis=0)


def beside(a, b):
    return jnp.concatenate([a, b], axis=1)


def barrier(devices, meanwhile):
    semaphore = pltpu.get_barrier_semaphore()
    for device in devices:
        pl.semaphore_signal(semaphore, inc=1, device_id=device, device_id_type=MESH)
    meanwhile()
    pl.semaphore_wait(semaphore, len(devices))


def remote(source, target, sent, received, device):
    return pltpu.make_async_remote_copy(
        src_ref=source, dst_ref=target, send_sem=sent, recv_sem=received, device_id=device, device_id_type=MESH
    )


class Place:
    def __init__(self):
        self.nx, self.nz = lax.axis_size("x"), lax.axis_size("z")
        self.x, self.z, self.core = lax.axis_index("x"), lax.axis_index("z"), lax.axis_index("core")
        chips = self.nx * self.nz
        self.chip = self.x * self.nz + self.z
        following, before = lax.rem(self.chip + 1, chips), lax.rem(self.chip + chips - 1, chips)
        self.following = {"x": following // self.nz, "z": lax.rem(following, self.nz)}
        self.before = {"x": before // self.nz, "z": lax.rem(before, self.nz)}
        self.partner = {"core": 1 - self.core}
        self.first = self.chip == 0
        self.last = self.chip == chips - 1

    def z_peers(self):
        return [{"z": lax.rem(self.z + d, self.nz)} for d in range(1, self.nz)]

    def x_peers(self):
        return [{"x": lax.rem(self.x + d, self.nx)} for d in range(1, self.nx)]

    def y_peers(self):
        return [{"y": lax.rem(lax.axis_index("y") + d, 4)} for d in range(1, 4)]

    def greet(self, meanwhile):
        barrier([self.partner, self.following, self.before] + self.z_peers() + self.x_peers() + self.y_peers(), meanwhile)


ABOVE = 2 * NB
OWN = 8 * NB
HALF = NB // 2


def sweeps_kernel(
    order_ref, offsets_ref, eig_ref, vt_ref, t_ref, out_ref,
    blocks_ref, own_ref, other_ref, mh_ref, ml_ref, resp_ref, re_ref, head_ref, next_ref,
    tz_ref, tx_ref, reach_ref, pzh_ref, pzl_ref, pxh_ref, pxl_ref, eh_ref, el_ref,
    rows_ref, turn_ref, turned_ref, edge_ref, edges_ref, sums_ref, totals_ref, ends_ref, y_ref,
    sent_y, received_y, sent_m, received_m, sent_n, received_n, sent_tz, received_tz, sent_tx, received_tx,
    sent, received, sent_z, received_z, sent_x, received_x, sent_h, received_h,
):
    here = Place()
    nx, nz, core, y = here.nx, here.nz, here.core, lax.axis_index("y")
    sweeps = vt_ref.shape[0]
    far = sorted(range(1, nz), key=lambda d: -min(d, nz - d))

    def own_block(p):
        stored = order_ref[p]
        blocks_ref[y, p, :NB] = vt_ref[stored]
        blocks_ref[y, p, NB:] = packed(t_ref[stored])

    def local_start():
        mine = eig_ref[...]
        turned = jnp.where(core == 0, mine, pltpu.roll(mine, NB, 1))
        turn_ref[0] = packed(turned[:, NB:])
        y_ref[: 4 * NB] = turned[:, :NB]
        for p in range(sweeps):
            own_block(p)
        rows_ref[...] = jnp.zeros_like(rows_ref)

    here.greet(local_start)

    def arrived(target, send_sem, recv_sem):
        remote(target, target, send_sem, recv_sem, here.partner).wait_recv()


    def block_copy(p, d):
        at = blocks_ref.at[y, p]
        return remote(at, at, sent_y.at[p, d], received_y.at[p, y], {"y": lax.rem(y + d, 4)})

    def map_copy(p):
        return remote(own_ref.at[p], other_ref.at[p], sent_m.at[p], received_m.at[p], here.partner)

    def head_copy(p):
        return remote(head_ref.at[p], next_ref.at[p], sent_n.at[p], received_n.at[p], here.before)

    def along_z(ref, p, d, send_sems, recv_sems):
        at = ref.at[p, here.z]
        return remote(at, at, send_sems.at[p, d], recv_sems.at[p, here.z], {"z": lax.rem(here.z + d, nz)})

    def along_x(ref, p, d, send_sems, recv_sems):
        at = ref.at[p, here.x]
        return remote(at, at, send_sems.at[p, d], recv_sems.at[p, here.x], {"x": lax.rem(here.x + d, nx)})

    def edge_copy(p):
        return remote(edge_ref.at[p], edges_ref.at[p], sent_h.at[p], received_h.at[p], here.before)

    def await_z(ref, p, send_sems, recv_sems):
        for d in range(1, nz):
            slot = lax.rem(here.z + d, nz)
            arrived(ref.at[p, slot], send_sems.at[p, d], recv_sems.at[p, slot])

    def await_x(ref, p, send_sems, recv_sems):
        for d in range(1, nx):
            slot = lax.rem(here.x + d, nx)
            arrived(ref.at[p, slot], send_sems.at[p, d], recv_sems.at[p, slot])


    eye = (lax.broadcasted_iota(jnp.int32, (NB, NB), 0) == lax.broadcasted_iota(jnp.int32, (NB, NB), 1)).astype(F32)
    wide_eye = (
        lax.broadcasted_iota(jnp.int32, (2 * NB, 2 * NB), 0) == lax.broadcasted_iota(jnp.int32, (2 * NB, 2 * NB), 1)
    ).astype(F32)

    def give(p):
        for d in (2, 1, 3):
            block_copy(p, d).start()

    def build(p):
        for d in range(1, 4):
            slot = lax.rem(y + d, 4)
            arrived(blocks_ref.at[slot, p], sent_y.at[p, d], received_y.at[p, slot])
        if p + 1 < sweeps:
            give(p + 1)
        maps = []
        for j in range(4):
            vt = blocks_ref[j, p, :NB]
            t = unpacked(blocks_ref[j, p, NB:])
            vh, vl = halves(vt)
            w = dot3(*halves(t), vh, vl)
            left = jnp.concatenate([vh, vh, vl], axis=0)
            product = lax.dot_general(
                left, three_below(w), (((0,), (0,)), ((), ())), preferred_element_type=F32
            )
            maps.append(wide_eye - product)
        carry = None
        for j in range(4):
            block = maps[j]
            rows = block if j == 0 else beside(dot_split(block[:, :NB], carry), block[:, NB:])
            done = jnp.concatenate([rows[:NB], jnp.zeros((NB, 6 * NB - rows.shape[1]), F32)], axis=1)
            own_ref[p, NB * j : NB * (j + 1), :] = done
            carry = rows[NB:]
        own_ref[p, 4 * NB :, :] = beside(carry, jnp.zeros((NB, NB), F32))
        map_copy(p).start()

    def respond(p):
        arrived(other_ref.at[p], sent_m.at[p], received_m.at[p])
        mine_first, other_first = own_ref[p, :, : 2 * NB], other_ref[p, :, : 2 * NB]
        first = jnp.where(core == 0, mine_first, other_first)[:, :NB]
        second = jnp.where(core == 0, other_first, mine_first)[:, :NB]
        later = dot_split(second, first[4 * NB :])
        tz_ref[p, here.z] = packed(later[4 * NB :])
        for d in far:
            along_z(tz_ref, p, d, sent_tz, received_tz).start()
        head_ref[p] = packed(first[: 2 * NB])
        head_copy(p).start()
        resp_ref[p] = later[4 * NB :]
        mine_last, other_last = own_ref[p, 4 * NB :, :], other_ref[p, 4 * NB :, :]
        end_first = jnp.where(core == 0, mine_last, other_last)
        end_second = jnp.where(core == 0, other_last, mine_last)
        through = dot_split(end_second[:, :NB], end_first)
        eh_ref[p], el_ref[p] = halves(jnp.concatenate([through[:, : 5 * NB], end_second[:, NB : 5 * NB]], axis=1))
        re_ref[p, : 4 * NB] = three_terms(first[: 4 * NB])
        re_ref[p, 4 * NB : 8 * NB] = three_terms(later[: 4 * NB])
        mh_ref[1 - core, p], ml_ref[1 - core, p] = halves(other_ref[p])
        mh_ref[core, p], ml_ref[core, p] = halves(own_ref[p])

    def chain_z(p):
        await_z(tz_ref, p, sent_tz, received_tz)
        both = jnp.concatenate([jnp.zeros((NB, NB), F32), eye], axis=0)
        upper = lax.broadcasted_iota(jnp.int32, (2 * NB, NB), 0) < NB
        twice = jnp.concatenate([eye, eye], axis=0)
        for slot in reversed(range(nz)):
            if slot < nz - 1:
                both = dot_split(both, unpacked(tz_ref[p, slot + 1]))
            both = jnp.where(jnp.logical_and(upper, slot == here.z - 1), twice, both)
            high, low = halves(both)
            at = slice(HALF * slot, HALF * (slot + 1))
            for ref, part in ((pzh_ref, high), (pzl_ref, low)):
                ref[p, :NB, at] = part[NB:, :HALF]
                ref[p, NB : 2 * NB, at] = part[NB:, HALF:]
                ref[p, 2 * NB : 3 * NB, at] = part[:NB, :HALF]
                ref[p, 3 * NB :, at] = part[:NB, HALF:]
        both = dot_split(both, unpacked(tz_ref[p, 0]))
        tx_ref[p, here.x] = packed(both[NB:])
        for d in range(1, nx):
            along_x(tx_ref, p, d, sent_tx, received_tx).start()
        reach_ref[p] = jnp.where(here.z == 0, eye, both[:NB])

    def ahead_of(p):
        arrived(next_ref.at[p], sent_n.at[p], received_n.at[p])
        ahead = unpacked(next_ref[p])
        ahead_high, ahead_low = halves(ahead)
        re_ref[p, 8 * NB :] = three_terms(dot3(ahead_high, ahead_low, *halves(resp_ref[p])))
        y_ref[8 * NB :] = dot3(ahead_high, ahead_low, *halves(unpacked(sums_ref[p, here.z])))

    def chain_x(p):
        await_x(tx_ref, p, sent_tx, received_tx)
        upto = jnp.zeros((NB, NB), F32)
        for slot in reversed(range(nx)):
            if slot < nx - 1:
                upto = dot_split(upto, unpacked(tx_ref[p, slot + 1]))
            upto = jnp.where(slot == here.x - 1, reach_ref[p], upto)
            high, low = halves(upto)
            at = slice(HALF * slot, HALF * (slot + 1))
            for ref, part in ((pxh_ref, high), (pxl_ref, low)):
                ref[p, :NB, at] = part[:, :HALF]
                ref[p, NB:, at] = part[:, HALF:]


    give(0)
    to_partner = remote(turn_ref.at[0], turned_ref.at[0], sent.at[0], received.at[0], here.partner)
    to_partner.start()

    kept = y_ref[: 4 * NB]
    arrived(turned_ref.at[0], sent.at[0], received.at[0])
    got = unpacked(turned_ref[0])
    rows_ref[ABOVE : ABOVE + OWN] = jnp.concatenate(
        [jnp.where(core == 0, kept, got), jnp.where(core == 0, got, kept)], axis=0
    )
    edge_ref[sweeps] = packed(rows_ref[ABOVE : ABOVE + 2 * NB])
    edge_copy(sweeps).start()
    build(0)
    respond(0)
    arrived(edges_ref.at[sweeps], sent_h.at[sweeps], received_h.at[sweeps])
    rows_ref[ABOVE + OWN : ABOVE + OWN + 2 * NB] = unpacked(edges_ref[sweeps])

    index = lax.broadcasted_iota(jnp.int32, (10 * NB, NB), 0)

    def sweep(p, before):
        offset = offsets_ref[order_ref[p]]
        shift = offset - before
        window = rows_ref[pl.ds(NB + shift, 10 * NB), :]
        beyond = jnp.logical_and(here.last, index >= 9 * NB - offset)
        carried = jnp.logical_and(jnp.logical_not(here.first), jnp.logical_and(index >= NB, index < 2 * NB))
        inputs = jnp.where(jnp.logical_or(beyond, carried), 0.0, window)
        head = window[:NB]
        high, low = halves(inputs[NB:])
        sums_ref[p, here.z] = packed(dot3(eh_ref[p], el_ref[p], high, low))
        for d in far:
            along_z(sums_ref, p, d, sent_z, received_z).start()
        high_a, low_a = high[: 6 * NB], low[: 6 * NB]
        body_a = dot3(mh_ref[0, p, : 4 * NB], ml_ref[0, p, : 4 * NB], high_a, low_a)
        edge_ref[p] = packed(body_a[: 2 * NB])
        edge_copy(p).start()
        rows_ref[NB:ABOVE] = head
        y_ref[: 4 * NB] = body_a
        end_a = dot3(mh_ref[0, p, 4 * NB :], ml_ref[0, p, 4 * NB :], high_a, low_a)
        second = jnp.concatenate([end_a, inputs[6 * NB :], jnp.zeros((NB, NB), F32)], axis=0)
        y_ref[4 * NB : 8 * NB] = dot3(mh_ref[1, p, : 4 * NB], ml_ref[1, p, : 4 * NB], *halves(second))
        if p == 0:
            build(1)
        chain_z(p)
        if p + 1 < sweeps:
            respond(p + 1)
        ahead_of(p)

        await_z(sums_ref, p, sent_z, received_z)
        high_z, low_z = halves(sums_ref[p].reshape(nz * HALF, 2 * NB))
        both = dot3(pzh_ref[p, : 2 * NB], pzl_ref[p, : 2 * NB], high_z, low_z)
        totals_ref[p, here.x] = packed(both[:NB, :NB] + both[NB:, NB:])
        for d in sorted(range(1, nx), key=lambda d: -min(d, nx - d)):
            along_x(totals_ref, p, d, sent_x, received_x).start()
        both = dot3(pzh_ref[p, 2 * NB :], pzl_ref[p, 2 * NB :], high_z, low_z)
        near = both[:NB, :NB] + both[NB:, NB:]
        if p + 2 < sweeps:
            build(p + 2)
        chain_x(p)
        arrived(edges_ref.at[p], sent_h.at[p], received_h.at[p])
        y_ref[8 * NB :] = unpacked(edges_ref[p]) + y_ref[8 * NB :]

        await_x(totals_ref, p, sent_x, received_x)
        high_x, low_x = halves(totals_ref[p].reshape(nx * HALF, 2 * NB))
        both = dot3(pxh_ref[p], pxl_ref[p], high_x, low_x)
        carry = near + both[:NB, :NB] + both[NB:, NB:]
        rows_ref[ABOVE : ABOVE + 10 * NB] = y_ref[...] + jnp.dot(
            re_ref[p], three_below(carry), preferred_element_type=F32
        )
        return offset

    last_offset = jnp.int32(0)
    for p in range(sweeps):
        last_offset = sweep(p, last_offset)


    ends_ref[0] = packed(rows_ref[ABOVE + 7 * NB : ABOVE + 8 * NB])
    to_next = remote(ends_ref.at[0], ends_ref.at[1], sent.at[1], received.at[1], here.following)
    to_next.start()

    def finish(p, _):
        for d in range(1, 4):
            block_copy(p, d).wait_send()
        map_copy(p).wait_send()
        head_copy(p).wait_send()
        edge_copy(p).wait_send()
        for d in range(1, nz):
            along_z(tz_ref, p, d, sent_tz, received_tz).wait_send()
            along_z(sums_ref, p, d, sent_z, received_z).wait_send()
        for d in range(1, nx):
            along_x(tx_ref, p, d, sent_tx, received_tx).wait_send()
            along_x(totals_ref, p, d, sent_x, received_x).wait_send()
        return 0

    lax.fori_loop(0, sweeps, finish, 0)
    edge_copy(sweeps).wait_send()
    to_partner.wait_send()
    arrived(ends_ref.at[1], sent.at[1], received.at[1])
    rows_ref[NB:ABOVE] = jnp.where(here.first, rows_ref[NB:ABOVE], unpacked(ends_ref[1]))
    final = rows_ref[pl.ds(ABOVE - last_offset, OWN), :]
    upper, lower = final[: 4 * NB], final[4 * NB :]
    turn_ref[1] = packed(jnp.where(core == 0, lower, upper))
    back = remote(turn_ref.at[1], turned_ref.at[1], sent.at[2], received.at[2], here.partner)
    back.start()
    kept = jnp.where(core == 0, upper, lower)
    arrived(turned_ref.at[1], sent.at[2], received.at[2])
    got = unpacked(turned_ref[1])
    out_ref[...] = beside(jnp.where(core == 0, kept, got), jnp.where(core == 0, got, kept))
    to_next.wait_send()
    back.wait_send()


def apply_sweeps(order, offsets, eigvecs, transposed, factors, nx, nz):
    sweeps = order.shape[0]
    dma = pltpu.SemaphoreType.DMA
    maps = (sweeps, 5 * NB, 6 * NB)
    full = (sweeps, NB, 2 * NB)
    scratch = [
        VM((4, sweeps, NB + HALF, 2 * NB), F32),
        VM(maps, F32),
        VM(maps, F32),
        VM((2,) + maps, BF16),
        VM((2,) + maps, BF16),
        VM((sweeps, NB, NB), F32),
        VM((sweeps, 10 * NB, 3 * NB), BF16),
        VM(full, F32),
        VM(full, F32),
        VM((sweeps, nz, HALF, 2 * NB), F32),
        VM((sweeps, nx, HALF, 2 * NB), F32),
        VM((sweeps, NB, NB), F32),
        VM((sweeps, 4 * NB, HALF * nz), BF16),
        VM((sweeps, 4 * NB, HALF * nz), BF16),
        VM((sweeps, 2 * NB, HALF * nx), BF16),
        VM((sweeps, 2 * NB, HALF * nx), BF16),
        VM((sweeps, NB, 9 * NB), BF16),
        VM((sweeps, NB, 9 * NB), BF16),
        VM((14 * NB, NB), F32),
        VM((2, 2 * NB, 2 * NB), F32),
        VM((2, 2 * NB, 2 * NB), F32),
        VM((sweeps + 1, NB, 2 * NB), F32),
        VM((sweeps + 1, NB, 2 * NB), F32),
        VM((sweeps, nz, HALF, 2 * NB), F32),
        VM((sweeps, nx, HALF, 2 * NB), F32),
        VM((2, HALF, 2 * NB), F32),
        VM((10 * NB, NB), F32),
        dma((sweeps, 4)),
        dma((sweeps, 4)),
        dma((sweeps,)),
        dma((sweeps,)),
        dma((sweeps,)),
        dma((sweeps,)),
        dma((sweeps, nz)),
        dma((sweeps, nz)),
        dma((sweeps, nx)),
        dma((sweeps, nx)),
        dma((3,)),
        dma((3,)),
        dma((sweeps, nz)),
        dma((sweeps, nz)),
        dma((sweeps, nx)),
        dma((sweeps, nx)),
        dma((sweeps + 1,)),
        dma((sweeps + 1,)),
    ]
    scalar, vector = pl.BlockSpec(memory_space=pltpu.SMEM), pl.BlockSpec(memory_space=VM)
    return pl.pallas_call(
        sweeps_kernel,
        out_shape=jax.ShapeDtypeStruct(eigvecs.shape, F32),
        in_specs=[scalar] * 2 + [vector] * 3,
        out_specs=vector,
        scratch_shapes=scratch,
        compiler_params=pltpu.CompilerParams(
            collective_id=0, has_side_effects=True, vmem_limit_bytes=60 * 1024 * 1024
        ),
        name="apply_sweeps",
    )(order, offsets, eigvecs, transposed, factors)


def solution(mesh):
    nz, cores, ny = 8, 2, mesh.shape["col"]
    nx = mesh.shape["row"] // (nz * cores)
    torus = Mesh(mesh.devices.reshape(nx, nz, cores, ny), ROW_COL)

    def local(eigvecs, reflectors, factors, order, offsets):
        transposed = jnp.swapaxes(reflectors[:, 0], 1, 2)
        return apply_sweeps(order, offsets, eigvecs, transposed, factors[:, 0], nx, nz)

    placed = (P(ROW, "y"), P(None, ROW_COL, None, None), P(None, ROW_COL, None, None), P(), P())
    return jax.shard_map(local, mesh=torus, in_specs=placed, out_specs=P(ROW, "y"), check_vma=False)
```
